32 devices in a mesh: dp: 8 (over z, y), rep: 4 (over x, core).
Axes of the slice: x: 2, y: 2, z: 4, core: 2. Of those that a mesh axis runs over, the one named last changes fastest.
Arguments:
- grads: bfloat16 [4, 8, 128, 4096], P('rep', 'dp')
- check_weights: int32 [4, 8, 8, 16], P('rep', 'dp'), may hold values from 1 to 8
Outputs:
- reduced: bfloat16 [128, 4096], P(None, 'dp')
- checksums: bfloat16 [8, 4096], P(None, 'dp')
The draws below stay inside these ranges and needn't reach their ends.
All inputs are finite; a program needn't handle non-finite values.
Results may differ from the reference program's by a relative error of at most 0.0039.
Values may be sent and summed in bfloat16 or wider, within the bound.
No kernel may reach another device: no remote copies, remote signals or barrier semaphores. Data moves between devices by JAX's collectives and lax.ppermute only.
A program may use at most 64 MiB of HBM per device.

```python
import jax
import jax.numpy as jnp
from jax import lax

D = 4096
ROWS = 128
BLOCK = 16
BLOCKS = 8
DPS = 8
REPS = 4


def draw_grads(key, part):
    first, second = jax.random.split(jax.random.fold_in(key, 11), 2)
    shape = (REPS, DPS, ROWS, D)
    ramp = 1.0 + 2.0 * jnp.arange(D, dtype=jnp.float32) / (D - 1)
    spread = jax.random.uniform(second, (D,), jnp.float32, 0.7, 1.4)
    values = jax.random.normal(first, shape, jnp.float32) * (ramp * spread)
    return values.astype(jnp.bfloat16)


def place_ends(values, stream_key, smallest, top_value):
    shape = values.shape
    index_at = [jax.random.randint(jax.random.fold_in(stream_key, axis), (), 0, shape[axis]) for axis in range(len(shape))]
    values = values.at[tuple(index_at)].set(smallest)
    longest = shape.index(max(shape))
    index_at[longest] = (index_at[longest] + 1) % shape[longest]
    return values.at[tuple(index_at)].set(top_value)


def setup_inputs(seed: int = 0) -> dict:
    keys = jax.random.split(jax.random.key(seed), 3)
    return {
        "grads": draw_grads(jax.random.fold_in(keys[2], 71), 0),
        "check_weights": place_ends(jax.random.randint(keys[1], (REPS, DPS, BLOCKS, BLOCK), 1, 9), jax.random.fold_in(keys[1], 1), 1, 8).astype(jnp.int32),
    }


def reference(grads, check_weights):

    def add_group(carry, pair):
        block, weights = pair
        wsum = lax.optimization_barrier(jnp.sum(weights, axis=-1)).astype(jnp.float32)
        data = block.astype(jnp.float32)
        shaped = data.reshape(data.shape[0], BLOCKS, BLOCK, data.shape[-1])
        local = jnp.einsum('dkb,dkbe->dke', weights.astype(jnp.float32), shaped)
        local = local / wsum[:, :, None]
        return ((carry[0] + lax.optimization_barrier(jnp.sum(data, axis=0)), carry[1] + lax.optimization_barrier(jnp.sum(local, axis=0))), None)
    start = (jnp.zeros((ROWS, D), jnp.float32), jnp.zeros((BLOCKS, D), jnp.float32))
    (summed, check_sum), unused = lax.scan(add_group, start, (grads, check_weights))
    square = jnp.sum(summed * summed)
    factor = jnp.minimum(1.0, 2.0 * jnp.sqrt(jnp.float32(ROWS * D)) / jnp.sqrt(square + 1e-06))
    return ((factor * summed).astype(jnp.bfloat16), (factor * check_sum).astype(jnp.bfloat16))
```

```python
import functools

import jax
import jax.numpy as jnp
from jax import lax
from jax.experimental import pallas as pl
from jax.experimental.pallas import tpu as pltpu
from jax.sharding import PartitionSpec as P

LANES = 128
SUBLANES = 8
GRANT = pltpu.CompilerParams(vmem_limit_bytes=8 * 1024 * 1024)


def clip_factor(square, total_rows, width):
    return jnp.minimum(
        1.0, 2.0 * jnp.sqrt(jnp.float32(total_rows * width)) / jnp.sqrt(square + 1e-06)
    )


def pack_kernel(grads_ref, weights_ref, out_ref, sem):
    parts, _, cols = out_ref.shape
    rows = grads_ref.shape[0]
    blocks, block = weights_ref.shape
    copies = [
        pltpu.make_async_copy(
            grads_ref.at[:, pl.ds(part * cols, cols)], out_ref.at[part, pl.ds(0, rows), :], sem
        )
        for part in range(parts)
    ]
    for copy in copies:
        copy.start()
    place = lax.broadcasted_iota(jnp.int32, (block, rows), 1)
    spread = (place % block == lax.broadcasted_iota(jnp.int32, (block, rows), 0)).astype(jnp.bfloat16)
    repeated = jnp.dot(
        weights_ref[...].astype(jnp.bfloat16), spread, preferred_element_type=jnp.float32
    )
    owner = lax.broadcasted_iota(jnp.int32, (blocks, rows), 1) // block
    mine = owner == lax.broadcasted_iota(jnp.int32, (blocks, rows), 0)
    diagonal = jnp.where(mine, repeated, 0.0).astype(jnp.bfloat16)
    for part in range(parts):
        out_ref[part, pl.ds(rows, blocks), :] = diagonal
    for copy in copies:
        copy.wait()


def sum_kernel(rows, recv_ref, total_ref, square_ref):
    parts, held, cols = recv_ref.shape
    blocks = held - rows
    total = jnp.zeros((rows, cols), jnp.float32)
    check = jnp.zeros((4 * blocks, cols), jnp.float32)
    for part in range(parts):
        data = recv_ref[part, pl.ds(0, rows), :]
        total += data.astype(jnp.float32)
        weights = recv_ref[part, pl.ds(rows, blocks), :].astype(jnp.float32)
        share = weights / jnp.sum(weights, axis=1, keepdims=True)
        high = share.astype(jnp.bfloat16).astype(jnp.float32)
        rest = share - high
        middle = rest.astype(jnp.bfloat16).astype(jnp.float32)
        low = rest - middle
        terms = jnp.concatenate([high, middle, low, jnp.zeros_like(low)], axis=0)
        check += jnp.dot(terms.astype(jnp.bfloat16), data, preferred_element_type=jnp.float32)
    total_ref[pl.ds(0, rows), :] = total
    total_ref[pl.ds(rows, blocks), :] = (
        check[:blocks] + check[blocks : 2 * blocks] + check[2 * blocks : 3 * blocks]
    )
    square_ref[...] = jnp.broadcast_to(
        jnp.sum(total * total, axis=0, keepdims=True), square_ref.shape
    )


def scale_kernel(rows, width, squares_ref, *refs):
    *total_refs, reduced_ref, check_ref = refs
    cols = total_refs[0].shape[1]
    factor = clip_factor(jnp.sum(squares_ref[...], keepdims=True), rows, width)
    me = lax.axis_index("rep")
    for step, total_ref in enumerate(total_refs):
        at = pl.ds(pl.multiple_of((me ^ step) * cols, cols), cols)
        scaled = (total_ref[...] * factor).astype(jnp.bfloat16)
        reduced_ref[:, at] = scaled[:rows]
        check_ref[:, at] = scaled[rows:]


def small_body(replicas, parts, grads, check_weights):
    local, weights = grads[0, 0], check_weights[0, 0]
    rows, width = local.shape
    blocks = weights.shape[0]
    cols = width // parts
    vmem = pl.BlockSpec(memory_space=pltpu.VMEM)
    packed = pl.pallas_call(
        pack_kernel,
        out_shape=jax.ShapeDtypeStruct((parts, rows + blocks, cols), jnp.bfloat16),
        in_specs=[pl.BlockSpec(memory_space=pl.ANY), vmem],
        out_specs=vmem,
        scratch_shapes=[pltpu.SemaphoreType.DMA],
        compiler_params=GRANT,
        name="pack",
    )(local, weights)
    received = lax.all_to_all(packed, ("dp", "rep"), 0, 0, tiled=True)
    total, square = pl.pallas_call(
        functools.partial(sum_kernel, rows),
        out_shape=(
            jax.ShapeDtypeStruct((rows + blocks, cols), jnp.float32),
            jax.ShapeDtypeStruct((parts, cols), jnp.float32),
        ),
        in_specs=[vmem],
        out_specs=(vmem, vmem),
        compiler_params=GRANT,
        name="add_up",
    )(received)
    totals = [total]
    for step in range(1, replicas):
        totals.append(lax.ppermute(total, "rep", [(i, i ^ step) for i in range(replicas)]))
    squares = lax.all_to_all(square, ("dp", "rep"), 0, 0, tiled=True)
    return pl.pallas_call(
        functools.partial(scale_kernel, rows, width),
        out_shape=(
            jax.ShapeDtypeStruct((rows, replicas * cols), jnp.bfloat16),
            jax.ShapeDtypeStruct((blocks, replicas * cols), jnp.bfloat16),
        ),
        in_specs=[vmem] * (1 + replicas),
        out_specs=(vmem, vmem),
        compiler_params=GRANT,
        name="scale",
    )(squares, *totals)


def large_body(grads, check_weights):
    local, weights = grads[0, 0], check_weights[0, 0]
    rows, width = local.shape
    blocks, block = weights.shape
    wsum = jnp.sum(weights, axis=-1).astype(jnp.float32)
    local_check = jnp.einsum(
        "kb,kbe->ke",
        weights.astype(jnp.bfloat16),
        local.reshape(blocks, block, width),
        preferred_element_type=jnp.float32,
    )
    terms = jnp.concatenate([local.astype(jnp.float32), local_check / wsum[:, None]], axis=0)
    owned = lax.psum(lax.psum_scatter(terms, "dp", scatter_dimension=1, tiled=True), "rep")
    square = lax.psum(jnp.sum(owned[:rows] * owned[:rows]), "dp")
    scaled = (clip_factor(square, rows, width) * owned).astype(jnp.bfloat16)
    return scaled[:rows], scaled[rows:]


def solution(mesh):
    replicas = mesh.shape["rep"]
    parts = replicas * mesh.shape["dp"]
    placed = P("rep", "dp", None, None)

    def step(grads, check_weights):
        rows, width = grads.shape[2:]
        blocks = check_weights.shape[2]
        tiled = (
            width == parts * LANES
            and rows == LANES
            and blocks == SUBLANES
            and replicas & (replicas - 1) == 0
        )
        body = functools.partial(small_body, replicas, parts) if tiled else large_body
        return jax.shard_map(
            body,
            mesh=mesh,
            in_specs=(placed, placed),
            out_specs=(P(None, "dp"), P(None, "dp")),
            check_vma=False,
        )(grads, check_weights)

    return step
```

```python
import functools

import jax
import jax.numpy as jnp
from jax import lax
from jax.experimental import pallas as pl
from jax.experimental.pallas import tpu as pltpu
from jax.sharding import Mesh
from jax.sharding import PartitionSpec as P

LANES = 128
SUBLANES = 8
GRANT = pltpu.CompilerParams(vmem_limit_bytes=8 * 1024 * 1024)


def clip_factor(square, total_rows, width):
    return jnp.minimum(
        1.0, 2.0 * jnp.sqrt(jnp.float32(total_rows * width)) / jnp.sqrt(square + 1e-06)
    )


def pack_kernel(grads_hbm, weights_hbm, out_ref, weights_ref, grads_sem, weights_sem):
    parts, held, cols = out_ref.shape
    rows, width = grads_hbm.shape
    blocks, block = weights_ref.shape
    halves = width // (parts * cols)
    fetch = pltpu.make_async_copy(weights_hbm, weights_ref, weights_sem)
    fetch.start()
    copies = [
        pltpu.make_async_copy(
            grads_hbm.at[:, pl.ds((half * parts + part) * cols, cols)],
            out_ref.at[part, pl.ds(half * rows, rows), :],
            grads_sem,
        )
        for half in range(halves)
        for part in range(parts)
    ]
    for copy in copies:
        copy.start()
    fetch.wait()
    place = lax.broadcasted_iota(jnp.int32, (block, rows), 1)
    spread = (place % block == lax.broadcasted_iota(jnp.int32, (block, rows), 0)).astype(jnp.bfloat16)
    repeated = jnp.dot(
        weights_ref[...].astype(jnp.bfloat16), spread, preferred_element_type=jnp.float32
    )
    owner = lax.broadcasted_iota(jnp.int32, (blocks, rows), 1) // block
    mine = owner == lax.broadcasted_iota(jnp.int32, (blocks, rows), 0)
    diagonal = jnp.where(mine, repeated, 0.0).astype(jnp.bfloat16)
    for part in range(parts):
        out_ref[part, pl.ds(held - blocks, blocks), :] = diagonal
    for copy in copies:
        copy.wait()


def sum_kernel(rows, recv_ref, mine_ref, other_ref):
    parts, held, cols = recv_ref.shape
    blocks = mine_ref.shape[0] - rows
    me = lax.axis_index("far")
    places = (me, 1 - me)
    totals = [jnp.zeros((rows, cols), jnp.float32)] * 2
    checks = [jnp.zeros((4 * blocks, cols), jnp.float32)] * 2
    for part in range(parts):
        weights = recv_ref[part, pl.ds(held - blocks, blocks), :].astype(jnp.float32)
        share = weights / jnp.sum(weights, axis=1, keepdims=True)
        high = share.astype(jnp.bfloat16).astype(jnp.float32)
        rest = share - high
        middle = rest.astype(jnp.bfloat16).astype(jnp.float32)
        low = rest - middle
        terms = jnp.concatenate([high, middle, low, jnp.zeros_like(low)], axis=0)
        terms = terms.astype(jnp.bfloat16)
        for i, place in enumerate(places):
            data = recv_ref[part, pl.ds(pl.multiple_of(place * rows, rows), rows), :]
            totals[i] += data.astype(jnp.float32)
            checks[i] += jnp.dot(terms, data, preferred_element_type=jnp.float32)
    for ref, total, check in zip((mine_ref, other_ref), totals, checks, strict=True):
        ref[pl.ds(0, rows), :] = total
        ref[pl.ds(rows, blocks), :] = (
            check[:blocks] + check[blocks : 2 * blocks] + check[2 * blocks : 3 * blocks]
        )


def join_kernel(rows, mine_ref, came_ref, total_ref, square_ref):
    total = mine_ref[...] + came_ref[...]
    total_ref[...] = total
    square_ref[...] = jnp.broadcast_to(
        jnp.sum(total[:rows] * total[:rows], axis=0, keepdims=True), square_ref.shape
    )


def scale_kernel(rows, width, squares_ref, *refs):
    *total_refs, reduced_ref, check_ref = refs
    cols = total_refs[0].shape[1]
    factor = clip_factor(jnp.sum(squares_ref[...], keepdims=True), rows, width)
    me = lax.axis_index("rep")
    for step, total_ref in enumerate(total_refs):
        at = pl.ds(pl.multiple_of((me ^ step) * cols, cols), cols)
        scaled = (total_ref[...] * factor).astype(jnp.bfloat16)
        reduced_ref[:, at] = scaled[:rows]
        check_ref[:, at] = scaled[rows:]


def small_body(sizes, grads, check_weights):
    far, near, replicas = sizes
    local, weights = grads[0, 0], check_weights[0, 0]
    rows, width = local.shape
    blocks = weights.shape[0]
    parts = near * replicas
    cols = width // (far * parts)
    vmem = pl.BlockSpec(memory_space=pltpu.VMEM)
    hbm = pl.BlockSpec(memory_space=pltpu.HBM)
    sums = jax.ShapeDtypeStruct((rows + blocks, cols), jnp.float32)
    packed = pl.pallas_call(
        pack_kernel,
        out_shape=jax.ShapeDtypeStruct((parts, far * rows + blocks, cols), jnp.bfloat16),
        in_specs=[hbm, hbm],
        out_specs=vmem,
        scratch_shapes=[
            pltpu.VMEM(weights.shape, weights.dtype),
            pltpu.SemaphoreType.DMA,
            pltpu.SemaphoreType.DMA,
        ],
        compiler_params=GRANT,
        name="pack",
    )(local, weights)
    received = lax.all_to_all(packed, ("near", "rep"), 0, 0, tiled=True)
    mine, other = pl.pallas_call(
        functools.partial(sum_kernel, rows),
        out_shape=(sums, sums),
        in_specs=[vmem],
        out_specs=(vmem, vmem),
        compiler_params=GRANT,
        name="add_up",
    )(received)
    came = lax.ppermute(other, "far", [(0, 1), (1, 0)])
    total, square = pl.pallas_call(
        functools.partial(join_kernel, rows),
        out_shape=(sums, jax.ShapeDtypeStruct((far * parts, cols), jnp.float32)),
        in_specs=[vmem, vmem],
        out_specs=(vmem, vmem),
        compiler_params=GRANT,
        name="join",
    )(mine, came)
    totals = [total]
    for step in range(1, replicas):
        totals.append(lax.ppermute(total, "rep", [(i, i ^ step) for i in range(replicas)]))
    squares = lax.all_to_all(square, ("far", "near", "rep"), 0, 0, tiled=True)
    return pl.pallas_call(
        functools.partial(scale_kernel, rows, width),
        out_shape=(
            jax.ShapeDtypeStruct((rows, replicas * cols), jnp.bfloat16),
            jax.ShapeDtypeStruct((blocks, replicas * cols), jnp.bfloat16),
        ),
        in_specs=[vmem] * (1 + replicas),
        out_specs=(vmem, vmem),
        compiler_params=GRANT,
        name="scale",
    )(squares, *totals)


def large_body(grads, check_weights):
    local, weights = grads[0, 0], check_weights[0, 0]
    rows, width = local.shape
    blocks, block = weights.shape
    wsum = jnp.sum(weights, axis=-1).astype(jnp.float32)
    local_check = jnp.einsum(
        "kb,kbe->ke",
        weights.astype(jnp.bfloat16),
        local.reshape(blocks, block, width),
        preferred_element_type=jnp.float32,
    )
    terms = jnp.concatenate([local.astype(jnp.float32), local_check / wsum[:, None]], axis=0)
    owned = lax.psum(lax.psum_scatter(terms, "dp", scatter_dimension=1, tiled=True), "rep")
    square = lax.psum(jnp.sum(owned[:rows] * owned[:rows]), "dp")
    scaled = (clip_factor(square, rows, width) * owned).astype(jnp.bfloat16)
    return scaled[:rows], scaled[rows:]


def solution(mesh):
    replicas, columns = mesh.shape["rep"], mesh.shape["dp"]
    far, near = 2, columns // 2

    def step(grads, check_weights):
        rows, width = grads.shape[2:]
        blocks = check_weights.shape[2]
        tiled = (
            width == columns * replicas * LANES
            and rows == LANES
            and blocks == SUBLANES
            and columns % far == 0
            and replicas & (replicas - 1) == 0
        )
        if tiled:
            body = functools.partial(small_body, (far, near, replicas))
            used = Mesh(mesh.devices.reshape(far, near, replicas), ("far", "near", "rep"))
            dp = ("far", "near")
        else:
            body, used, dp = large_body, mesh, "dp"
        placed = P("rep", dp, None, None)
        return jax.shard_map(
            body,
            mesh=used,
            in_specs=(placed, placed),
            out_specs=(P(None, dp), P(None, dp)),
            check_vma=False,
        )(grads, check_weights)

    return step
```

```python
import functools

import jax
import jax.numpy as jnp
from jax import lax
from jax.experimental import pallas as pl
from jax.experimental.pallas import tpu as pltpu
from jax.sharding import Mesh
from jax.sharding import PartitionSpec as P

LANES = 128
SUBLANES = 8
GRANT = pltpu.CompilerParams(vmem_limit_bytes=8 * 1024 * 1024)


def clip_factor(square, total_rows, width):
    return jnp.minimum(
        1.0, 2.0 * jnp.sqrt(jnp.float32(total_rows * width)) / jnp.sqrt(square + 1e-06)
    )


def pack_kernel(grads_hbm, weights_hbm, out_ref, weights_ref, grads_sem, weights_sem):
    parts, held, cols = out_ref.shape
    rows, width = grads_hbm.shape
    blocks, block = weights_ref.shape
    halves = width // (parts * cols)
    fetch = pltpu.make_async_copy(weights_hbm, weights_ref, weights_sem)
    fetch.start()
    copies = [
        pltpu.make_async_copy(
            grads_hbm.at[:, pl.ds((half * parts + part) * cols, cols)],
            out_ref.at[part, pl.ds(half * rows, rows), :],
            grads_sem,
        )
        for half in range(halves)
        for part in range(parts)
    ]
    for copy in copies:
        copy.start()
    fetch.wait()
    place = lax.broadcasted_iota(jnp.int32, (block, rows), 1)
    spread = (place % block == lax.broadcasted_iota(jnp.int32, (block, rows), 0)).astype(jnp.bfloat16)
    repeated = jnp.dot(
        weights_ref[...].astype(jnp.bfloat16), spread, preferred_element_type=jnp.float32
    )
    owner = lax.broadcasted_iota(jnp.int32, (blocks, rows), 1) // block
    mine = owner == lax.broadcasted_iota(jnp.int32, (blocks, rows), 0)
    diagonal = jnp.where(mine, repeated, 0.0).astype(jnp.bfloat16)
    for part in range(parts):
        out_ref[part, pl.ds(held - blocks, blocks), :] = diagonal
    for copy in copies:
        copy.wait()


def sum_other_kernel(rows, recv_ref, sums_ref, shares_ref):
    parts, held, _ = recv_ref.shape
    blocks = sums_ref.shape[0] - rows
    for part in range(parts):
        weights = recv_ref[part, pl.ds(held - blocks, blocks), :].astype(jnp.float32)
        share = weights / jnp.sum(weights, axis=1, keepdims=True)
        high = share.astype(jnp.bfloat16).astype(jnp.float32)
        rest = share - high
        middle = rest.astype(jnp.bfloat16).astype(jnp.float32)
        low = rest - middle
        terms = jnp.concatenate([high, middle, low, jnp.zeros_like(low)], axis=0)
        shares_ref[part] = terms.astype(jnp.bfloat16)
    add_up(rows, 1 - lax.axis_index("far"), recv_ref, shares_ref, sums_ref)


def sum_mine_kernel(rows, recv_ref, shares_ref, sums_ref):
    add_up(rows, lax.axis_index("far"), recv_ref, shares_ref, sums_ref)


def add_up(rows, half, recv_ref, shares_ref, sums_ref):
    parts, _, cols = recv_ref.shape
    blocks = sums_ref.shape[0] - rows
    total = jnp.zeros((rows, cols), jnp.float32)
    check = jnp.zeros((4 * blocks, cols), jnp.float32)
    at = pl.ds(pl.multiple_of(half * rows, rows), rows)
    for part in range(parts):
        data = recv_ref[part, at, :]
        total += data.astype(jnp.float32)
        check += jnp.dot(shares_ref[part], data, preferred_element_type=jnp.float32)
    sums_ref[pl.ds(0, rows), :] = total
    sums_ref[pl.ds(rows, blocks), :] = (
        check[:blocks] + check[blocks : 2 * blocks] + check[2 * blocks : 3 * blocks]
    )


def join_kernel(rows, mine_ref, came_ref, total_ref, square_ref):
    total = mine_ref[...] + came_ref[...]
    total_ref[...] = total
    square_ref[...] = jnp.broadcast_to(
        jnp.sum(total[:rows] * total[:rows], axis=0, keepdims=True), square_ref.shape
    )


def scale_kernel(rows, width, squares_ref, *refs):
    *total_refs, reduced_ref, check_ref = refs
    cols = total_refs[0].shape[1]
    factor = clip_factor(jnp.sum(squares_ref[...], keepdims=True), rows, width)
    me = lax.axis_index("rep")
    for step, total_ref in enumerate(total_refs):
        at = pl.ds(pl.multiple_of((me ^ step) * cols, cols), cols)
        scaled = (total_ref[...] * factor).astype(jnp.bfloat16)
        reduced_ref[:, at] = scaled[:rows]
        check_ref[:, at] = scaled[rows:]


def small_body(sizes, grads, check_weights):
    far, near, replicas = sizes
    local, weights = grads[0, 0], check_weights[0, 0]
    rows, width = local.shape
    blocks = weights.shape[0]
    parts = near * replicas
    cols = width // (far * parts)
    vmem = pl.BlockSpec(memory_space=pltpu.VMEM)
    hbm = pl.BlockSpec(memory_space=pltpu.HBM)
    sums = jax.ShapeDtypeStruct((rows + blocks, cols), jnp.float32)
    packed = pl.pallas_call(
        pack_kernel,
        out_shape=jax.ShapeDtypeStruct((parts, far * rows + blocks, cols), jnp.bfloat16),
        in_specs=[hbm, hbm],
        out_specs=vmem,
        scratch_shapes=[
            pltpu.VMEM(weights.shape, weights.dtype),
            pltpu.SemaphoreType.DMA,
            pltpu.SemaphoreType.DMA,
        ],
        compiler_params=GRANT,
        name="pack",
    )(
        pltpu.with_memory_space_constraint(local, pltpu.HBM),
        pltpu.with_memory_space_constraint(weights, pltpu.HBM),
    )
    received = lax.all_to_all(packed, ("near", "rep"), 0, 0, tiled=True)
    other, shares = pl.pallas_call(
        functools.partial(sum_other_kernel, rows),
        out_shape=(sums, jax.ShapeDtypeStruct((parts, 4 * blocks, rows), jnp.bfloat16)),
        in_specs=[vmem],
        out_specs=(vmem, vmem),
        compiler_params=GRANT,
        name="sum_other",
    )(received)
    came = lax.ppermute(other, "far", [(0, 1), (1, 0)])
    mine = pl.pallas_call(
        functools.partial(sum_mine_kernel, rows),
        out_shape=sums,
        in_specs=[vmem, vmem],
        out_specs=vmem,
        compiler_params=GRANT,
        name="sum_mine",
    )(received, shares)
    total, square = pl.pallas_call(
        functools.partial(join_kernel, rows),
        out_shape=(sums, jax.ShapeDtypeStruct((far * parts, cols), jnp.float32)),
        in_specs=[vmem, vmem],
        out_specs=(vmem, vmem),
        compiler_params=GRANT,
        name="join",
    )(mine, came)
    totals = [total]
    for step in range(1, replicas):
        totals.append(lax.ppermute(total, "rep", [(i, i ^ step) for i in range(replicas)]))
    squares = lax.all_to_all(square, ("far", "near", "rep"), 0, 0, tiled=True)
    return pl.pallas_call(
        functools.partial(scale_kernel, rows, width),
        out_shape=(
            jax.ShapeDtypeStruct((rows, replicas * cols), jnp.bfloat16),
            jax.ShapeDtypeStruct((blocks, replicas * cols), jnp.bfloat16),
        ),
        in_specs=[vmem] * (1 + replicas),
        out_specs=(vmem, vmem),
        compiler_params=GRANT,
        name="scale",
    )(squares, *totals)


def large_body(grads, check_weights):
    local, weights = grads[0, 0], check_weights[0, 0]
    rows, width = local.shape
    blocks, block = weights.shape
    wsum = jnp.sum(weights, axis=-1).astype(jnp.float32)
    local_check = jnp.einsum(
        "kb,kbe->ke",
        weights.astype(jnp.bfloat16),
        local.reshape(blocks, block, width),
        preferred_element_type=jnp.float32,
    )
    terms = jnp.concatenate([local.astype(jnp.float32), local_check / wsum[:, None]], axis=0)
    owned = lax.psum(lax.psum_scatter(terms, "dp", scatter_dimension=1, tiled=True), "rep")
    square = lax.psum(jnp.sum(owned[:rows] * owned[:rows]), "dp")
    scaled = (clip_factor(square, rows, width) * owned).astype(jnp.bfloat16)
    return scaled[:rows], scaled[rows:]


def solution(mesh):
    replicas, columns = mesh.shape["rep"], mesh.shape["dp"]
    far, near = 2, columns // 2

    def step(grads, check_weights):
        rows, width = grads.shape[2:]
        blocks = check_weights.shape[2]
        tiled = (
            width == columns * replicas * LANES
            and rows == LANES
            and blocks == SUBLANES
            and columns % far == 0
            and replicas & (replicas - 1) == 0
        )
        if tiled:
            body = functools.partial(small_body, (far, near, replicas))
            used = Mesh(mesh.devices.reshape(far, near, replicas), ("far", "near", "rep"))
            dp = ("far", "near")
        else:
            body, used, dp = large_body, mesh, "dp"
        placed = P("rep", dp, None, None)
        return jax.shard_map(
            body,
            mesh=used,
            in_specs=(placed, placed),
            out_specs=(P(None, dp), P(None, dp)),
            check_vma=False,
        )(grads, check_weights)

    return step
```

```python
import functools

import jax
import jax.numpy as jnp
from jax import lax
from jax.experimental import pallas as pl
from jax.experimental.pallas import tpu as pltpu
from jax.sharding import Mesh
from jax.sharding import PartitionSpec as P

LANES = 128
SUBLANES = 8
FULL = 32767.0
LEAST, MOST = -110, 126
GRANT = pltpu.CompilerParams(vmem_limit_bytes=8 * 1024 * 1024)


def clip_factor(square, total_rows, width):
    return jnp.minimum(
        1.0, 2.0 * jnp.sqrt(jnp.float32(total_rows * width)) / jnp.sqrt(square + 1e-06)
    )


def pack_kernel(mine, grads_hbm, weights_hbm, out_ref, weights_ref, grads_sem, weights_sem):
    core = lax.axis_index("core")
    target = core if mine else 1 - core
    rows, width = grads_hbm.shape
    blocks, block = weights_ref.shape
    cols = out_ref.shape[1]
    chips = width // (4 * cols)
    fetch = pltpu.make_async_copy(weights_hbm, weights_ref, weights_sem)
    fetch.start()
    copies = []
    for chip in range(chips):
        for half in range(2):
            at = pl.multiple_of(((half * chips + chip) * 2 + target) * cols, cols)
            copies.append(
                pltpu.make_async_copy(
                    grads_hbm.at[:, pl.ds(at, cols)],
                    out_ref.at[pl.ds((chip * 2 + half) * rows, rows), :],
                    grads_sem,
                )
            )
            copies[-1].start()
    fetch.wait()
    place = lax.broadcasted_iota(jnp.int32, (block, rows), 1)
    spread = (place % block == lax.broadcasted_iota(jnp.int32, (block, rows), 0)).astype(jnp.bfloat16)
    repeated = jnp.dot(
        weights_ref[...].astype(jnp.bfloat16), spread, preferred_element_type=jnp.float32
    )
    owner = lax.broadcasted_iota(jnp.int32, (blocks, rows), 1) // block
    own = owner == lax.broadcasted_iota(jnp.int32, (blocks, rows), 0)
    out_ref[pl.ds(2 * chips * rows, blocks), :] = jnp.where(own, repeated, 0.0).astype(jnp.bfloat16)
    for copy in copies:
        copy.wait()


def encode(values):
    top = jnp.maximum(jnp.max(jnp.abs(values), axis=0, keepdims=True), 2.0**LEAST)
    power = jnp.clip(jnp.ceil(jnp.log2(top)), float(LEAST), float(MOST))
    codes = jnp.round(values * (jnp.exp2(-power) * FULL))
    return jnp.clip(codes, -FULL, FULL).astype(jnp.int32), power.astype(jnp.int32)


def decode(codes, power):
    return codes.astype(jnp.int32).astype(jnp.float32) * (
        jnp.exp2(power.astype(jnp.float32)) * (1.0 / FULL)
    )


def shares_of(weights):
    weights = weights.astype(jnp.float32)
    share = weights / jnp.sum(weights, axis=1, keepdims=True)
    high = share.astype(jnp.bfloat16).astype(jnp.float32)
    rest = share - high
    middle = rest.astype(jnp.bfloat16).astype(jnp.float32)
    low = rest - middle
    terms = jnp.concatenate([high, middle, low, jnp.zeros_like(low)], axis=0)
    return terms.astype(jnp.bfloat16)


def pair_kernel(rows, mine_ref, came_ref, out_ref):
    chips, held, cols = out_ref.shape
    blocks = mine_ref.shape[0] - 2 * chips * rows
    weights = pl.ds(2 * chips * rows, blocks)
    shares = shares_of(mine_ref[weights, :]), shares_of(came_ref[weights, :])
    for chip in range(chips):
        powers = []
        for half in range(2):
            at = pl.ds((chip * 2 + half) * rows, rows)
            first, second = mine_ref[at, :], came_ref[at, :]
            check = jnp.dot(shares[0], first, preferred_element_type=jnp.float32)
            check += jnp.dot(shares[1], second, preferred_element_type=jnp.float32)
            check = check[:blocks] + check[blocks : 2 * blocks] + check[2 * blocks : 3 * blocks]
            codes, power = encode(first.astype(jnp.float32) + second.astype(jnp.float32))
            out_ref[chip, pl.ds(half * (rows + blocks), rows), :] = codes.astype(jnp.int16)
            powers.append(power)
            codes, power = encode(check)
            out_ref[chip, pl.ds(half * (rows + blocks) + rows, blocks), :] = codes.astype(jnp.int16)
            powers.append(power)
        powers.append(jnp.zeros((SUBLANES - 4, cols), jnp.int32))
        out_ref[chip, pl.ds(held - SUBLANES, SUBLANES), :] = jnp.concatenate(powers, axis=0).astype(
            jnp.int16
        )


def add_up(rows, blocks, half, recv_ref):
    chips, held, cols = recv_ref.shape
    total = jnp.zeros((rows, cols), jnp.float32)
    check = jnp.zeros((blocks, cols), jnp.float32)
    start = pl.multiple_of(half * (rows + blocks), SUBLANES)
    for chip in range(chips):
        powers = recv_ref[chip, pl.ds(held - SUBLANES, SUBLANES), :].astype(jnp.int32)
        powers = jnp.where(half == 0, powers[:2], powers[2:4])
        total += decode(recv_ref[chip, pl.ds(start, rows), :], powers[:1])
        check += decode(recv_ref[chip, pl.ds(start + rows, blocks), :], powers[1:])
    return total, check


def sum_other_kernel(rows, blocks, recv_ref, out_ref):
    total, check = add_up(rows, blocks, 1 - lax.axis_index("far"), recv_ref)
    codes, power = encode(total)
    out_ref[pl.ds(0, rows), :] = codes.astype(jnp.int16)
    codes, check_power = encode(check)
    out_ref[pl.ds(rows, blocks), :] = codes.astype(jnp.int16)
    rest = jnp.zeros((SUBLANES - 2, power.shape[1]), jnp.int32)
    out_ref[pl.ds(rows + blocks, SUBLANES), :] = jnp.concatenate(
        [power, check_power, rest], axis=0
    ).astype(jnp.int16)


def sum_mine_kernel(rows, blocks, recv_ref, sums_ref):
    total, check = add_up(rows, blocks, lax.axis_index("far"), recv_ref)
    sums_ref[pl.ds(0, rows), :] = total
    sums_ref[pl.ds(rows, blocks), :] = check


def join_kernel(rows, blocks, mine_ref, came_ref, total_ref, square_ref):
    powers = came_ref[pl.ds(rows + blocks, SUBLANES), :].astype(jnp.int32)
    total = mine_ref[pl.ds(0, rows), :] + decode(came_ref[pl.ds(0, rows), :], powers[:1])
    total_ref[pl.ds(0, rows), :] = total
    total_ref[pl.ds(rows, blocks), :] = mine_ref[pl.ds(rows, blocks), :] + decode(
        came_ref[pl.ds(rows, blocks), :], powers[1:2]
    )
    square_ref[...] = jnp.broadcast_to(
        jnp.sum(total * total, axis=0, keepdims=True), square_ref.shape
    )


def scale_kernel(rows, width, squares_ref, *refs):
    *total_refs, reduced_ref, check_ref = refs
    cols = total_refs[0].shape[1]
    factor = clip_factor(jnp.sum(squares_ref[...], keepdims=True), rows, width)
    me = lax.axis_index("side") * 2 + lax.axis_index("core")
    for step, total_ref in enumerate(total_refs):
        at = pl.ds(pl.multiple_of((me ^ step) * cols, cols), cols)
        scaled = (total_ref[...] * factor).astype(jnp.bfloat16)
        reduced_ref[:, at] = scaled[:rows]
        check_ref[:, at] = scaled[rows:]


def small_body(sizes, grads, check_weights):
    far, near, side, core = sizes
    local, weights = grads[0, 0], check_weights[0, 0]
    rows, width = local.shape
    blocks = weights.shape[0]
    chips, replicas = near * side, side * core
    cols = width // (far * chips * core)
    vmem = pl.BlockSpec(memory_space=pltpu.VMEM)
    hbm = pl.BlockSpec(memory_space=pltpu.HBM)
    sums = jax.ShapeDtypeStruct((rows + blocks, cols), jnp.float32)
    local = pltpu.with_memory_space_constraint(local, pltpu.HBM)
    weights = pltpu.with_memory_space_constraint(weights, pltpu.HBM)

    def pack(mine):
        return pl.pallas_call(
            functools.partial(pack_kernel, mine),
            out_shape=jax.ShapeDtypeStruct((far * chips * rows + blocks, cols), jnp.bfloat16),
            in_specs=[hbm, hbm],
            out_specs=vmem,
            scratch_shapes=[
                pltpu.VMEM(weights.shape, weights.dtype),
                pltpu.SemaphoreType.DMA,
                pltpu.SemaphoreType.DMA,
            ],
            compiler_params=GRANT,
        )(local, weights)

    def call(kernel, out_shape, *operands):
        return pl.pallas_call(
            kernel,
            out_shape=out_shape,
            in_specs=[vmem] * len(operands),
            out_specs=jax.tree.map(lambda _: vmem, out_shape),
            compiler_params=GRANT,
        )(*operands)

    packed = pack(False)
    came = lax.ppermute(packed, "core", [(0, 1), (1, 0)])
    mine = pack(True)
    coded = call(
        functools.partial(pair_kernel, rows),
        jax.ShapeDtypeStruct((chips, far * (rows + blocks) + SUBLANES, cols), jnp.int16),
        mine,
        came,
    )
    received = lax.all_to_all(coded, ("near", "side"), 0, 0, tiled=True)
    other = call(
        functools.partial(sum_other_kernel, rows, blocks),
        jax.ShapeDtypeStruct((rows + blocks + SUBLANES, cols), jnp.int16),
        received,
    )
    came = lax.ppermute(other, "far", [(0, 1), (1, 0)])
    mine = call(functools.partial(sum_mine_kernel, rows, blocks), sums, received)
    total, square = call(
        functools.partial(join_kernel, rows, blocks),
        (sums, jax.ShapeDtypeStruct((far * chips * core, cols), jnp.float32)),
        mine,
        came,
    )
    totals = [total]
    for step in range(1, replicas):
        swaps = [(i, i ^ step) for i in range(replicas)]
        totals.append(lax.ppermute(total, ("side", "core"), swaps))
    squares = lax.all_to_all(square, ("far", "near", "side", "core"), 0, 0, tiled=True)
    wide = replicas * cols
    return call(
        functools.partial(scale_kernel, rows, width),
        (
            jax.ShapeDtypeStruct((rows, wide), jnp.bfloat16),
            jax.ShapeDtypeStruct((blocks, wide), jnp.bfloat16),
        ),
        squares,
        *totals,
    )


def large_body(grads, check_weights):
    local, weights = grads[0, 0], check_weights[0, 0]
    rows, width = local.shape
    blocks, block = weights.shape
    wsum = jnp.sum(weights, axis=-1).astype(jnp.float32)
    local_check = jnp.einsum(
        "kb,kbe->ke",
        weights.astype(jnp.bfloat16),
        local.reshape(blocks, block, width),
        preferred_element_type=jnp.float32,
    )
    terms = jnp.concatenate([local.astype(jnp.float32), local_check / wsum[:, None]], axis=0)
    owned = lax.psum(lax.psum_scatter(terms, "dp", scatter_dimension=1, tiled=True), "rep")
    square = lax.psum(jnp.sum(owned[:rows] * owned[:rows]), "dp")
    scaled = (clip_factor(square, rows, width) * owned).astype(jnp.bfloat16)
    return scaled[:rows], scaled[rows:]


def solution(mesh):
    replicas, columns = mesh.shape["rep"], mesh.shape["dp"]
    far, near, side, core = sizes = 2, columns // 2, replicas // 2, 2

    def step(grads, check_weights):
        rows, width = grads.shape[2:]
        blocks = check_weights.shape[2]
        tiled = (
            width == columns * replicas * LANES
            and rows == LANES
            and blocks == SUBLANES
            and columns == far * near
            and replicas == side * core
            and replicas & (replicas - 1) == 0
        )
        if tiled:
            axes = ("far", "near", "side", "core")
            body, used = functools.partial(small_body, sizes), Mesh(mesh.devices.reshape(sizes), axes)
            dp, rep = axes[:2], axes[2:]
        else:
            body, used, dp, rep = large_body, mesh, "dp", "rep"
        placed = P(rep, dp, None, None)
        return jax.shard_map(
            body,
            mesh=used,
            in_specs=(placed, placed),
            out_specs=(P(None, dp), P(None, dp)),
            check_vma=False,
        )(grads, check_weights)

    return step
```

```python
import functools

import jax
import jax.numpy as jnp
from jax import lax
from jax.experimental import pallas as pl
from jax.experimental.pallas import tpu as pltpu
from jax.sharding import Mesh
from jax.sharding import PartitionSpec as P

LANES = 128
SUBLANES = 8
FULL = 32767.0
LEAST, MOST = -126, 126
GRANT = pltpu.CompilerParams(vmem_limit_bytes=8 * 1024 * 1024)


def clip_factor(square, total_rows, width):
    return jnp.minimum(
        1.0, 2.0 * jnp.sqrt(jnp.float32(total_rows * width)) / jnp.sqrt(square + 1e-06)
    )


def pack_kernel(mine, grads_hbm, weights_hbm, out_ref, weights_ref, grads_sem, weights_sem):
    core = lax.axis_index("core")
    target = core if mine else 1 - core
    rows, width = grads_hbm.shape
    blocks, block = weights_ref.shape
    cols = out_ref.shape[1]
    chips = width // (4 * cols)
    fetch = pltpu.make_async_copy(weights_hbm, weights_ref, weights_sem)
    fetch.start()
    copies = []
    for chip in range(chips):
        for half in range(2):
            at = pl.multiple_of(((half * chips + chip) * 2 + target) * cols, cols)
            copies.append(
                pltpu.make_async_copy(
                    grads_hbm.at[:, pl.ds(at, cols)],
                    out_ref.at[pl.ds((chip * 2 + half) * rows, rows), :],
                    grads_sem,
                )
            )
            copies[-1].start()
    fetch.wait()
    place = lax.broadcasted_iota(jnp.int32, (block, rows), 1)
    spread = (place % block == lax.broadcasted_iota(jnp.int32, (block, rows), 0)).astype(jnp.bfloat16)
    repeated = jnp.dot(
        weights_ref[...].astype(jnp.bfloat16), spread, preferred_element_type=jnp.float32
    )
    owner = lax.broadcasted_iota(jnp.int32, (blocks, rows), 1) // block
    own = owner == lax.broadcasted_iota(jnp.int32, (blocks, rows), 0)
    out_ref[pl.ds(2 * chips * rows, blocks), :] = jnp.where(own, repeated, 0.0).astype(jnp.bfloat16)
    for copy in copies:
        copy.wait()


def encode(values):
    top = jnp.maximum(jnp.max(jnp.abs(values), axis=0, keepdims=True), 2.0**LEAST)
    power = jnp.clip(jnp.ceil(jnp.log2(top)), float(LEAST), float(MOST))
    codes = jnp.round(values * jnp.exp2(-power) * FULL)
    return jnp.clip(codes, -FULL, FULL).astype(jnp.int32), power.astype(jnp.int32)


def decode(codes, power):
    values = codes.astype(jnp.int32).astype(jnp.float32) * (1.0 / FULL)
    return values * jnp.exp2(power.astype(jnp.float32))


def shares_of(weights):
    weights = weights.astype(jnp.float32)
    share = weights / jnp.sum(weights, axis=1, keepdims=True)
    high = share.astype(jnp.bfloat16).astype(jnp.float32)
    rest = share - high
    middle = rest.astype(jnp.bfloat16).astype(jnp.float32)
    low = rest - middle
    terms = jnp.concatenate([high, middle, low, jnp.zeros_like(low)], axis=0)
    return terms.astype(jnp.bfloat16)


def pair_kernel(rows, mine_ref, came_ref, out_ref):
    chips, held, cols = out_ref.shape
    blocks = mine_ref.shape[0] - 2 * chips * rows
    weights = pl.ds(2 * chips * rows, blocks)
    shares = shares_of(mine_ref[weights, :]), shares_of(came_ref[weights, :])
    for chip in range(chips):
        powers = []
        for half in range(2):
            at = pl.ds((chip * 2 + half) * rows, rows)
            first, second = mine_ref[at, :], came_ref[at, :]
            check = jnp.dot(shares[0], first, preferred_element_type=jnp.float32)
            check += jnp.dot(shares[1], second, preferred_element_type=jnp.float32)
            check = check[:blocks] + check[blocks : 2 * blocks] + check[2 * blocks : 3 * blocks]
            codes, power = encode(first.astype(jnp.float32) + second.astype(jnp.float32))
            out_ref[chip, pl.ds(half * (rows + blocks), rows), :] = codes.astype(jnp.int16)
            powers.append(power)
            codes, power = encode(check)
            out_ref[chip, pl.ds(half * (rows + blocks) + rows, blocks), :] = codes.astype(jnp.int16)
            powers.append(power)
        powers.append(jnp.zeros((SUBLANES - 4, cols), jnp.int32))
        out_ref[chip, pl.ds(held - SUBLANES, SUBLANES), :] = jnp.concatenate(powers, axis=0).astype(
            jnp.int16
        )


def add_up(rows, blocks, half, recv_ref):
    chips, held, cols = recv_ref.shape
    total = jnp.zeros((rows, cols), jnp.float32)
    check = jnp.zeros((blocks, cols), jnp.float32)
    start = pl.multiple_of(half * (rows + blocks), SUBLANES)
    for chip in range(chips):
        powers = recv_ref[chip, pl.ds(held - SUBLANES, SUBLANES), :].astype(jnp.int32)
        powers = jnp.where(half == 0, powers[:2], powers[2:4])
        total += decode(recv_ref[chip, pl.ds(start, rows), :], powers[:1])
        check += decode(recv_ref[chip, pl.ds(start + rows, blocks), :], powers[1:])
    return total, check


def sum_other_kernel(rows, blocks, recv_ref, out_ref):
    total, check = add_up(rows, blocks, 1 - lax.axis_index("far"), recv_ref)
    codes, power = encode(total)
    out_ref[pl.ds(0, rows), :] = codes.astype(jnp.int16)
    codes, check_power = encode(check)
    out_ref[pl.ds(rows, blocks), :] = codes.astype(jnp.int16)
    rest = jnp.zeros((SUBLANES - 2, power.shape[1]), jnp.int32)
    out_ref[pl.ds(rows + blocks, SUBLANES), :] = jnp.concatenate(
        [power, check_power, rest], axis=0
    ).astype(jnp.int16)


def sum_mine_kernel(rows, blocks, recv_ref, sums_ref):
    total, check = add_up(rows, blocks, lax.axis_index("far"), recv_ref)
    sums_ref[pl.ds(0, rows), :] = total
    sums_ref[pl.ds(rows, blocks), :] = check


def join_kernel(rows, blocks, mine_ref, came_ref, total_ref, square_ref):
    powers = came_ref[pl.ds(rows + blocks, SUBLANES), :].astype(jnp.int32)
    total = mine_ref[pl.ds(0, rows), :] + decode(came_ref[pl.ds(0, rows), :], powers[:1])
    total_ref[pl.ds(0, rows), :] = total
    total_ref[pl.ds(rows, blocks), :] = mine_ref[pl.ds(rows, blocks), :] + decode(
        came_ref[pl.ds(rows, blocks), :], powers[1:2]
    )
    square_ref[...] = jnp.broadcast_to(
        jnp.sum(total * total, axis=0, keepdims=True), square_ref.shape
    )


def scale_kernel(rows, width, squares_ref, *refs):
    *total_refs, reduced_ref, check_ref = refs
    cols = total_refs[0].shape[1]
    factor = clip_factor(jnp.sum(squares_ref[...], keepdims=True), rows, width)
    me = lax.axis_index("side") * 2 + lax.axis_index("core")
    for step, total_ref in enumerate(total_refs):
        at = pl.ds(pl.multiple_of((me ^ step) * cols, cols), cols)
        scaled = (total_ref[...] * factor).astype(jnp.bfloat16)
        reduced_ref[:, at] = scaled[:rows]
        check_ref[:, at] = scaled[rows:]


def small_body(sizes, grads, check_weights):
    far, near, side, core = sizes
    local, weights = grads[0, 0], check_weights[0, 0]
    rows, width = local.shape
    blocks = weights.shape[0]
    chips, replicas = near * side, side * core
    cols = width // (far * chips * core)
    vmem = pl.BlockSpec(memory_space=pltpu.VMEM)
    hbm = pl.BlockSpec(memory_space=pltpu.HBM)
    sums = jax.ShapeDtypeStruct((rows + blocks, cols), jnp.float32)
    local = pltpu.with_memory_space_constraint(local, pltpu.HBM)
    weights = pltpu.with_memory_space_constraint(weights, pltpu.HBM)

    def pack(mine):
        return pl.pallas_call(
            functools.partial(pack_kernel, mine),
            out_shape=jax.ShapeDtypeStruct((far * chips * rows + blocks, cols), jnp.bfloat16),
            in_specs=[hbm, hbm],
            out_specs=vmem,
            scratch_shapes=[
                pltpu.VMEM(weights.shape, weights.dtype),
                pltpu.SemaphoreType.DMA,
                pltpu.SemaphoreType.DMA,
            ],
            compiler_params=GRANT,
        )(local, weights)

    def call(kernel, out_shape, *operands):
        return pl.pallas_call(
            kernel,
            out_shape=out_shape,
            in_specs=[vmem] * len(operands),
            out_specs=jax.tree.map(lambda _: vmem, out_shape),
            compiler_params=GRANT,
        )(*operands)

    packed = pack(False)
    came = lax.ppermute(packed, "core", [(0, 1), (1, 0)])
    mine = pack(True)
    coded = call(
        functools.partial(pair_kernel, rows),
        jax.ShapeDtypeStruct((chips, far * (rows + blocks) + SUBLANES, cols), jnp.int16),
        mine,
        came,
    )
    received = lax.all_to_all(coded, ("near", "side"), 0, 0, tiled=True)
    other = call(
        functools.partial(sum_other_kernel, rows, blocks),
        jax.ShapeDtypeStruct((rows + blocks + SUBLANES, cols), jnp.int16),
        received,
    )
    came = lax.ppermute(other, "far", [(0, 1), (1, 0)])
    mine = call(functools.partial(sum_mine_kernel, rows, blocks), sums, received)
    total, square = call(
        functools.partial(join_kernel, rows, blocks),
        (sums, jax.ShapeDtypeStruct((far * chips * core, cols), jnp.float32)),
        mine,
        came,
    )
    totals = [total]
    for step in range(1, replicas):
        swaps = [(i, i ^ step) for i in range(replicas)]
        totals.append(lax.ppermute(total, ("side", "core"), swaps))
    squares = lax.all_to_all(square, ("far", "near", "side", "core"), 0, 0, tiled=True)
    wide = replicas * cols
    return call(
        functools.partial(scale_kernel, rows, width),
        (
            jax.ShapeDtypeStruct((rows, wide), jnp.bfloat16),
            jax.ShapeDtypeStruct((blocks, wide), jnp.bfloat16),
        ),
        squares,
        *totals,
    )


def large_body(grads, check_weights):
    local, weights = grads[0, 0], check_weights[0, 0]
    rows, width = local.shape
    blocks, block = weights.shape
    wsum = jnp.sum(weights, axis=-1).astype(jnp.float32)
    local_check = jnp.einsum(
        "kb,kbe->ke",
        weights.astype(jnp.bfloat16),
        local.reshape(blocks, block, width),
        preferred_element_type=jnp.float32,
    )
    terms = jnp.concatenate([local.astype(jnp.float32), local_check / wsum[:, None]], axis=0)
    owned = lax.psum(lax.psum_scatter(terms, "dp", scatter_dimension=1, tiled=True), "rep")
    square = lax.psum(jnp.sum(owned[:rows] * owned[:rows]), "dp")
    scaled = (clip_factor(square, rows, width) * owned).astype(jnp.bfloat16)
    return scaled[:rows], scaled[rows:]


def solution(mesh):
    replicas, columns = mesh.shape["rep"], mesh.shape["dp"]
    far, near, side, core = sizes = 2, columns // 2, replicas // 2, 2

    def step(grads, check_weights):
        rows, width = grads.shape[2:]
        blocks = check_weights.shape[2]
        tiled = (
            width == columns * replicas * LANES
            and rows == LANES
            and blocks == SUBLANES
            and columns == far * near
            and replicas == side * core
            and replicas & (replicas - 1) == 0
        )
        if tiled:
            axes = ("far", "near", "side", "core")
            body, used = functools.partial(small_body, sizes), Mesh(mesh.devices.reshape(sizes), axes)
            dp, rep = axes[:2], axes[2:]
        else:
            body, used, dp, rep = large_body, mesh, "dp", "rep"
        placed = P(rep, dp, None, None)
        return jax.shard_map(
            body,
            mesh=used,
            in_specs=(placed, placed),
            out_specs=(P(None, dp), P(None, dp)),
            check_vma=False,
        )(grads, check_weights)

    return step
```

```python
import functools

import jax
import jax.numpy as jnp
from jax import lax
from jax.experimental import pallas as pl
from jax.experimental.pallas import tpu as pltpu
from jax.sharding import Mesh
from jax.sharding import PartitionSpec as P

LANES = 128
SUBLANES = 8
FULL = 32767.0
LEAST, MOST = -126, 126
GRANT = pltpu.CompilerParams(vmem_limit_bytes=8 * 1024 * 1024)


def clip_factor(square, total_rows, width):
    return jnp.minimum(
        1.0, 2.0 * jnp.sqrt(jnp.float32(total_rows * width)) / jnp.sqrt(square + 1e-06)
    )


def pack_kernel(mine, grads_hbm, weights_hbm, out_ref, weights_ref, grads_sem, weights_sem):
    core = lax.axis_index("core")
    target = core if mine else 1 - core
    rows, width = grads_hbm.shape
    blocks, block = weights_ref.shape
    cols = out_ref.shape[1]
    chips = width // (4 * cols)
    fetch = pltpu.make_async_copy(weights_hbm, weights_ref, weights_sem)
    fetch.start()
    copies = []
    for chip in range(chips):
        for half in range(2):
            at = pl.multiple_of(((half * chips + chip) * 2 + target) * cols, cols)
            copies.append(
                pltpu.make_async_copy(
                    grads_hbm.at[:, pl.ds(at, cols)],
                    out_ref.at[pl.ds((chip * 2 + half) * rows, rows), :],
                    grads_sem,
                )
            )
            copies[-1].start()
    fetch.wait()
    place = lax.broadcasted_iota(jnp.int32, (block, rows), 1)
    spread = (place % block == lax.broadcasted_iota(jnp.int32, (block, rows), 0)).astype(jnp.bfloat16)
    repeated = jnp.dot(
        weights_ref[...].astype(jnp.bfloat16), spread, preferred_element_type=jnp.float32
    )
    owner = lax.broadcasted_iota(jnp.int32, (blocks, rows), 1) // block
    own = owner == lax.broadcasted_iota(jnp.int32, (blocks, rows), 0)
    out_ref[pl.ds(2 * chips * rows, blocks), :] = jnp.where(own, repeated, 0.0).astype(jnp.bfloat16)
    for copy in copies:
        copy.wait()


def encode(values):
    top = jnp.maximum(jnp.max(jnp.abs(values), axis=0, keepdims=True), 2.0**LEAST)
    power = jnp.clip(jnp.ceil(jnp.log2(top)), float(LEAST), float(MOST))
    codes = jnp.round(values * jnp.exp2(-power) * FULL)
    return jnp.clip(codes, -FULL, FULL).astype(jnp.int32), power.astype(jnp.int32)


def decode(codes, power):
    values = codes.astype(jnp.int32).astype(jnp.float32) * (1.0 / FULL)
    return values * jnp.exp2(power.astype(jnp.float32))


def shares_of(weights):
    weights = weights.astype(jnp.float32)
    share = weights / jnp.sum(weights, axis=1, keepdims=True)
    high = share.astype(jnp.bfloat16).astype(jnp.float32)
    rest = share - high
    middle = rest.astype(jnp.bfloat16).astype(jnp.float32)
    low = rest - middle
    terms = jnp.concatenate([high, middle, low, jnp.zeros_like(low)], axis=0)
    return terms.astype(jnp.bfloat16)


def pair_kernel(rows, mine_ref, came_ref, out_ref):
    chips, held, cols = out_ref.shape
    blocks = mine_ref.shape[0] - 2 * chips * rows
    weights = pl.ds(2 * chips * rows, blocks)
    shares = shares_of(mine_ref[weights, :]), shares_of(came_ref[weights, :])
    for chip in range(chips):
        powers = []
        for half in range(2):
            at = pl.ds((chip * 2 + half) * rows, rows)
            first, second = mine_ref[at, :], came_ref[at, :]
            check = jnp.dot(shares[0], first, preferred_element_type=jnp.float32)
            check += jnp.dot(shares[1], second, preferred_element_type=jnp.float32)
            check = check[:blocks] + check[blocks : 2 * blocks] + check[2 * blocks : 3 * blocks]
            codes, power = encode(first.astype(jnp.float32) + second.astype(jnp.float32))
            out_ref[chips - 1 - chip, pl.ds(half * (rows + blocks), rows), :] = codes.astype(jnp.int16)
            powers.append(power)
            codes, power = encode(check)
            out_ref[chips - 1 - chip, pl.ds(half * (rows + blocks) + rows, blocks), :] = codes.astype(jnp.int16)
            powers.append(power)
        powers.append(jnp.zeros((SUBLANES - 4, cols), jnp.int32))
        out_ref[chips - 1 - chip, pl.ds(held - SUBLANES, SUBLANES), :] = jnp.concatenate(powers, axis=0).astype(
            jnp.int16
        )


def add_up(rows, blocks, half, recv_ref):
    chips, held, cols = recv_ref.shape
    total = jnp.zeros((rows, cols), jnp.float32)
    check = jnp.zeros((blocks, cols), jnp.float32)
    start = pl.multiple_of(half * (rows + blocks), SUBLANES)
    for chip in range(chips):
        powers = recv_ref[chip, pl.ds(held - SUBLANES, SUBLANES), :].astype(jnp.int32)
        powers = jnp.where(half == 0, powers[:2], powers[2:4])
        total += decode(recv_ref[chip, pl.ds(start, rows), :], powers[:1])
        check += decode(recv_ref[chip, pl.ds(start + rows, blocks), :], powers[1:])
    return total, check


def sum_kernel(rows, blocks, recv_ref, out_ref, mine_ref, other_ref):
    far = lax.axis_index("far")
    other, other_check = add_up(rows, blocks, 1 - far, recv_ref)
    mine, mine_check = add_up(rows, blocks, far, recv_ref)
    powers, start = [], 0
    for values in (other, other_check, mine):
        codes, power = encode(values)
        out_ref[pl.ds(start, values.shape[0]), :] = codes.astype(jnp.int16)
        powers.append(power)
        start += values.shape[0]
    powers.append(jnp.zeros((SUBLANES - len(powers), out_ref.shape[1]), jnp.int32))
    out_ref[pl.ds(start, SUBLANES), :] = jnp.concatenate(powers, axis=0).astype(jnp.int16)
    mine_ref[pl.ds(0, rows), :] = mine
    mine_ref[pl.ds(rows, blocks), :] = mine_check
    other_ref[...] = other


def join_kernel(rows, blocks, mine_ref, other_ref, came_ref, total_ref, square_ref):
    held = rows + blocks
    powers = came_ref[pl.ds(held + rows, SUBLANES), :].astype(jnp.int32)
    total = mine_ref[pl.ds(0, rows), :] + decode(came_ref[pl.ds(0, rows), :], powers[:1])
    other = other_ref[...] + decode(came_ref[pl.ds(held, rows), :], powers[2:3])
    square_ref[...] = jnp.broadcast_to(
        jnp.sum(total * total + other * other, axis=0, keepdims=True), square_ref.shape
    )
    total_ref[pl.ds(0, rows), :] = total
    total_ref[pl.ds(rows, blocks), :] = mine_ref[pl.ds(rows, blocks), :] + decode(
        came_ref[pl.ds(rows, blocks), :], powers[1:2]
    )


def scale_kernel(rows, width, squares_ref, *refs):
    *total_refs, reduced_ref, check_ref = refs
    cols = total_refs[0].shape[1]
    factor = clip_factor(jnp.sum(squares_ref[...], keepdims=True), rows, width)
    me = lax.axis_index("side") * 2 + lax.axis_index("core")
    for step, total_ref in enumerate(total_refs):
        at = pl.ds(pl.multiple_of((me ^ step) * cols, cols), cols)
        scaled = (total_ref[...] * factor).astype(jnp.bfloat16)
        reduced_ref[:, at] = scaled[:rows]
        check_ref[:, at] = scaled[rows:]


def small_body(sizes, grads, check_weights):
    far, near, side, core = sizes
    local, weights = grads[0, 0], check_weights[0, 0]
    rows, width = local.shape
    blocks = weights.shape[0]
    chips, replicas = near * side, side * core
    cols = width // (far * chips * core)
    vmem = pl.BlockSpec(memory_space=pltpu.VMEM)
    hbm = pl.BlockSpec(memory_space=pltpu.HBM)
    sums = jax.ShapeDtypeStruct((rows + blocks, cols), jnp.float32)
    local = pltpu.with_memory_space_constraint(local, pltpu.HBM)
    weights = pltpu.with_memory_space_constraint(weights, pltpu.HBM)

    def pack(mine):
        return pl.pallas_call(
            functools.partial(pack_kernel, mine),
            out_shape=jax.ShapeDtypeStruct((far * chips * rows + blocks, cols), jnp.bfloat16),
            in_specs=[hbm, hbm],
            out_specs=vmem,
            scratch_shapes=[
                pltpu.VMEM(weights.shape, weights.dtype),
                pltpu.SemaphoreType.DMA,
                pltpu.SemaphoreType.DMA,
            ],
            compiler_params=GRANT,
        )(local, weights)

    def call(kernel, out_shape, *operands):
        return pl.pallas_call(
            kernel,
            out_shape=out_shape,
            in_specs=[vmem] * len(operands),
            out_specs=jax.tree.map(lambda _: vmem, out_shape),
            compiler_params=GRANT,
        )(*operands)

    packed = pack(False)
    came = lax.ppermute(packed, "core", [(0, 1), (1, 0)])
    mine = pack(True)
    coded = call(
        functools.partial(pair_kernel, rows),
        jax.ShapeDtypeStruct((chips, far * (rows + blocks) + SUBLANES, cols), jnp.int16),
        mine,
        came,
    )
    backward = [list(range(chips))[::-1]]
    received = lax.all_to_all(
        coded, ("near", "side"), 0, 0, tiled=True, axis_index_groups=backward
    )
    part = jax.ShapeDtypeStruct((rows, cols), jnp.float32)
    codes, mine, other = call(
        functools.partial(sum_kernel, rows, blocks),
        (jax.ShapeDtypeStruct((2 * rows + blocks + SUBLANES, cols), jnp.int16), sums, part),
        received,
    )
    came = lax.ppermute(codes, "far", [(0, 1), (1, 0)])
    total, square = call(
        functools.partial(join_kernel, rows, blocks),
        (sums, jax.ShapeDtypeStruct((chips * core, cols), jnp.float32)),
        mine,
        other,
        came,
    )
    totals = [total]
    for step in range(1, replicas):
        swaps = [(i, i ^ step) for i in range(replicas)]
        totals.append(lax.ppermute(total, ("side", "core"), swaps))
    backward = [list(range(chips * core))[::-1]]
    squares = lax.all_to_all(
        square, ("near", "side", "core"), 0, 0, tiled=True, axis_index_groups=backward
    )
    wide = replicas * cols
    return call(
        functools.partial(scale_kernel, rows, width),
        (
            jax.ShapeDtypeStruct((rows, wide), jnp.bfloat16),
            jax.ShapeDtypeStruct((blocks, wide), jnp.bfloat16),
        ),
        squares,
        *totals,
    )


def large_body(grads, check_weights):
    local, weights = grads[0, 0], check_weights[0, 0]
    rows, width = local.shape
    blocks, block = weights.shape
    wsum = jnp.sum(weights, axis=-1).astype(jnp.float32)
    local_check = jnp.einsum(
        "kb,kbe->ke",
        weights.astype(jnp.bfloat16),
        local.reshape(blocks, block, width),
        preferred_element_type=jnp.float32,
    )
    terms = jnp.concatenate([local.astype(jnp.float32), local_check / wsum[:, None]], axis=0)
    owned = lax.psum(lax.psum_scatter(terms, "dp", scatter_dimension=1, tiled=True), "rep")
    square = lax.psum(jnp.sum(owned[:rows] * owned[:rows]), "dp")
    scaled = (clip_factor(square, rows, width) * owned).astype(jnp.bfloat16)
    return scaled[:rows], scaled[rows:]


def solution(mesh):
    replicas, columns = mesh.shape["rep"], mesh.shape["dp"]
    far, near, side, core = sizes = 2, columns // 2, replicas // 2, 2

    def step(grads, check_weights):
        rows, width = grads.shape[2:]
        blocks = check_weights.shape[2]
        tiled = (
            width == columns * replicas * LANES
            and rows == LANES
            and blocks == SUBLANES
            and columns == far * near
            and replicas == side * core
            and replicas & (replicas - 1) == 0
        )
        if tiled:
            axes = ("far", "near", "side", "core")
            body, used = functools.partial(small_body, sizes), Mesh(mesh.devices.reshape(sizes), axes)
            dp, rep = axes[:2], axes[2:]
        else:
            body, used, dp, rep = large_body, mesh, "dp", "rep"
        placed = P(rep, dp, None, None)
        return jax.shard_map(
            body,
            mesh=used,
            in_specs=(placed, placed),
            out_specs=(P(None, dp), P(None, dp)),
            check_vma=False,
        )(grads, check_weights)

    return step
```

```python
import functools

import jax
import jax.numpy as jnp
from jax import lax
from jax.experimental import pallas as pl
from jax.experimental.pallas import tpu as pltpu
from jax.sharding import Mesh
from jax.sharding import PartitionSpec as P

LANES = 128
SUBLANES = 8
FULL = 32767.0
LEAST, MOST = -126, 126
GRANT = pltpu.CompilerParams(vmem_limit_bytes=8 * 1024 * 1024)


def clip_factor(square, total_rows, width):
    return jnp.minimum(
        1.0, 2.0 * jnp.sqrt(jnp.float32(total_rows * width)) / jnp.sqrt(square + 1e-06)
    )


def pack_kernel(mine, grads_hbm, weights_hbm, out_ref, weights_ref, grads_sem, weights_sem):
    core = lax.axis_index("core")
    target = core if mine else 1 - core
    rows, width = grads_hbm.shape
    blocks, block = weights_ref.shape
    cols = out_ref.shape[1]
    chips = width // (4 * cols)
    fetch = pltpu.make_async_copy(weights_hbm, weights_ref, weights_sem)
    fetch.start()
    copies = []
    for chip in range(chips):
        for half in range(2):
            at = pl.multiple_of(((half * chips + chip) * 2 + target) * cols, cols)
            copies.append(
                pltpu.make_async_copy(
                    grads_hbm.at[:, pl.ds(at, cols)],
                    out_ref.at[pl.ds((chip * 2 + half) * rows, rows), :],
                    grads_sem,
                )
            )
            copies[-1].start()
    fetch.wait()
    place = lax.broadcasted_iota(jnp.int32, (block, rows), 1)
    spread = (place % block == lax.broadcasted_iota(jnp.int32, (block, rows), 0)).astype(jnp.bfloat16)
    repeated = jnp.dot(
        weights_ref[...].astype(jnp.bfloat16), spread, preferred_element_type=jnp.float32
    )
    owner = lax.broadcasted_iota(jnp.int32, (blocks, rows), 1) // block
    own = owner == lax.broadcasted_iota(jnp.int32, (blocks, rows), 0)
    out_ref[pl.ds(2 * chips * rows, blocks), :] = jnp.where(own, repeated, 0.0).astype(jnp.bfloat16)
    for copy in copies:
        copy.wait()


def encode(values):
    top = jnp.maximum(jnp.max(jnp.abs(values), axis=0, keepdims=True), 2.0**LEAST)
    power = jnp.clip(jnp.ceil(jnp.log2(top)), float(LEAST), float(MOST))
    codes = jnp.round(values * jnp.exp2(-power) * FULL)
    return jnp.clip(codes, -FULL, FULL).astype(jnp.int32), power.astype(jnp.int32)


def decode(codes, power):
    values = codes.astype(jnp.int32).astype(jnp.float32) * (1.0 / FULL)
    return values * jnp.exp2(power.astype(jnp.float32))


def shares_of(weights):
    weights = weights.astype(jnp.float32)
    share = weights / jnp.sum(weights, axis=1, keepdims=True)
    high = share.astype(jnp.bfloat16).astype(jnp.float32)
    rest = share - high
    middle = rest.astype(jnp.bfloat16).astype(jnp.float32)
    low = rest - middle
    terms = jnp.concatenate([high, middle, low, jnp.zeros_like(low)], axis=0)
    return terms.astype(jnp.bfloat16)


def place_of(chip, chips):
    return chip ^ (chips - 2)


def pair_kernel(rows, mine_ref, came_ref, out_ref):
    chips, held, cols = out_ref.shape
    blocks = mine_ref.shape[0] - 2 * chips * rows
    weights = pl.ds(2 * chips * rows, blocks)
    shares = shares_of(mine_ref[weights, :]), shares_of(came_ref[weights, :])
    for chip in range(chips):
        powers = []
        for half in range(2):
            at = pl.ds((chip * 2 + half) * rows, rows)
            first, second = mine_ref[at, :], came_ref[at, :]
            check = jnp.dot(shares[0], first, preferred_element_type=jnp.float32)
            check += jnp.dot(shares[1], second, preferred_element_type=jnp.float32)
            check = check[:blocks] + check[blocks : 2 * blocks] + check[2 * blocks : 3 * blocks]
            codes, power = encode(first.astype(jnp.float32) + second.astype(jnp.float32))
            out_ref[place_of(chip, chips), pl.ds(half * (rows + blocks), rows), :] = codes.astype(jnp.int16)
            powers.append(power)
            codes, power = encode(check)
            out_ref[place_of(chip, chips), pl.ds(half * (rows + blocks) + rows, blocks), :] = codes.astype(jnp.int16)
            powers.append(power)
        powers.append(jnp.zeros((SUBLANES - 4, cols), jnp.int32))
        out_ref[place_of(chip, chips), pl.ds(held - SUBLANES, SUBLANES), :] = jnp.concatenate(powers, axis=0).astype(
            jnp.int16
        )


def add_up(rows, blocks, half, recv_ref):
    chips, held, cols = recv_ref.shape
    total = jnp.zeros((rows, cols), jnp.float32)
    check = jnp.zeros((blocks, cols), jnp.float32)
    start = pl.multiple_of(half * (rows + blocks), SUBLANES)
    for chip in range(chips):
        powers = recv_ref[chip, pl.ds(held - SUBLANES, SUBLANES), :].astype(jnp.int32)
        powers = jnp.where(half == 0, powers[:2], powers[2:4])
        total += decode(recv_ref[chip, pl.ds(start, rows), :], powers[:1])
        check += decode(recv_ref[chip, pl.ds(start + rows, blocks), :], powers[1:])
    return total, check


def sum_kernel(rows, blocks, recv_ref, out_ref, mine_ref, other_ref):
    far = lax.axis_index("far")
    other, other_check = add_up(rows, blocks, 1 - far, recv_ref)
    mine, mine_check = add_up(rows, blocks, far, recv_ref)
    powers, start = [], 0
    for values in (other, other_check, mine):
        codes, power = encode(values)
        out_ref[pl.ds(start, values.shape[0]), :] = codes.astype(jnp.int16)
        powers.append(power)
        start += values.shape[0]
    powers.append(jnp.zeros((SUBLANES - len(powers), out_ref.shape[1]), jnp.int32))
    out_ref[pl.ds(start, SUBLANES), :] = jnp.concatenate(powers, axis=0).astype(jnp.int16)
    mine_ref[pl.ds(0, rows), :] = mine
    mine_ref[pl.ds(rows, blocks), :] = mine_check
    other_ref[...] = other


def join_kernel(rows, blocks, mine_ref, other_ref, came_ref, total_ref, square_ref):
    held = rows + blocks
    powers = came_ref[pl.ds(held + rows, SUBLANES), :].astype(jnp.int32)
    total = mine_ref[pl.ds(0, rows), :] + decode(came_ref[pl.ds(0, rows), :], powers[:1])
    other = other_ref[...] + decode(came_ref[pl.ds(held, rows), :], powers[2:3])
    square_ref[...] = jnp.broadcast_to(
        jnp.sum(total * total + other * other, axis=0, keepdims=True), square_ref.shape
    )
    total_ref[pl.ds(0, rows), :] = total
    total_ref[pl.ds(rows, blocks), :] = mine_ref[pl.ds(rows, blocks), :] + decode(
        came_ref[pl.ds(rows, blocks), :], powers[1:2]
    )


def scale_kernel(rows, width, squares_ref, *refs):
    *total_refs, reduced_ref, check_ref = refs
    cols = total_refs[0].shape[1]
    factor = clip_factor(jnp.sum(squares_ref[...], keepdims=True), rows, width)
    me = lax.axis_index("side") * 2 + lax.axis_index("core")
    for step, total_ref in enumerate(total_refs):
        at = pl.ds(pl.multiple_of((me ^ step) * cols, cols), cols)
        scaled = (total_ref[...] * factor).astype(jnp.bfloat16)
        reduced_ref[:, at] = scaled[:rows]
        check_ref[:, at] = scaled[rows:]


def small_body(sizes, grads, check_weights):
    far, near, side, core = sizes
    local, weights = grads[0, 0], check_weights[0, 0]
    rows, width = local.shape
    blocks = weights.shape[0]
    chips, replicas = near * side, side * core
    cols = width // (far * chips * core)
    vmem = pl.BlockSpec(memory_space=pltpu.VMEM)
    hbm = pl.BlockSpec(memory_space=pltpu.HBM)
    sums = jax.ShapeDtypeStruct((rows + blocks, cols), jnp.float32)
    local = pltpu.with_memory_space_constraint(local, pltpu.HBM)
    weights = pltpu.with_memory_space_constraint(weights, pltpu.HBM)

    def pack(mine):
        return pl.pallas_call(
            functools.partial(pack_kernel, mine),
            out_shape=jax.ShapeDtypeStruct((far * chips * rows + blocks, cols), jnp.bfloat16),
            in_specs=[hbm, hbm],
            out_specs=vmem,
            scratch_shapes=[
                pltpu.VMEM(weights.shape, weights.dtype),
                pltpu.SemaphoreType.DMA,
                pltpu.SemaphoreType.DMA,
            ],
            compiler_params=GRANT,
        )(local, weights)

    def call(kernel, out_shape, *operands):
        return pl.pallas_call(
            kernel,
            out_shape=out_shape,
            in_specs=[vmem] * len(operands),
            out_specs=jax.tree.map(lambda _: vmem, out_shape),
            compiler_params=GRANT,
        )(*operands)

    packed = pack(False)
    came = lax.ppermute(packed, "core", [(0, 1), (1, 0)])
    mine = pack(True)
    coded = call(
        functools.partial(pair_kernel, rows),
        jax.ShapeDtypeStruct((chips, far * (rows + blocks) + SUBLANES, cols), jnp.int16),
        mine,
        came,
    )
    order = [[place_of(chip, chips) for chip in range(chips)]]
    received = lax.all_to_all(
        coded, ("near", "side"), 0, 0, tiled=True, axis_index_groups=order
    )
    part = jax.ShapeDtypeStruct((rows, cols), jnp.float32)
    codes, mine, other = call(
        functools.partial(sum_kernel, rows, blocks),
        (jax.ShapeDtypeStruct((2 * rows + blocks + SUBLANES, cols), jnp.int16), sums, part),
        received,
    )
    came = lax.ppermute(codes, "far", [(0, 1), (1, 0)])
    total, square = call(
        functools.partial(join_kernel, rows, blocks),
        (sums, jax.ShapeDtypeStruct((chips * core, cols), jnp.float32)),
        mine,
        other,
        came,
    )
    totals = [total]
    for step in range(1, replicas):
        swaps = [(i, i ^ step) for i in range(replicas)]
        totals.append(lax.ppermute(total, ("side", "core"), swaps))
    backward = [list(range(chips * core))[::-1]]
    squares = lax.all_to_all(
        square, ("near", "side", "core"), 0, 0, tiled=True, axis_index_groups=backward
    )
    wide = replicas * cols
    return call(
        functools.partial(scale_kernel, rows, width),
        (
            jax.ShapeDtypeStruct((rows, wide), jnp.bfloat16),
            jax.ShapeDtypeStruct((blocks, wide), jnp.bfloat16),
        ),
        squares,
        *totals,
    )


def large_body(grads, check_weights):
    local, weights = grads[0, 0], check_weights[0, 0]
    rows, width = local.shape
    blocks, block = weights.shape
    wsum = jnp.sum(weights, axis=-1).astype(jnp.float32)
    local_check = jnp.einsum(
        "kb,kbe->ke",
        weights.astype(jnp.bfloat16),
        local.reshape(blocks, block, width),
        preferred_element_type=jnp.float32,
    )
    terms = jnp.concatenate([local.astype(jnp.float32), local_check / wsum[:, None]], axis=0)
    owned = lax.psum(lax.psum_scatter(terms, "dp", scatter_dimension=1, tiled=True), "rep")
    square = lax.psum(jnp.sum(owned[:rows] * owned[:rows]), "dp")
    scaled = (clip_factor(square, rows, width) * owned).astype(jnp.bfloat16)
    return scaled[:rows], scaled[rows:]


def solution(mesh):
    replicas, columns = mesh.shape["rep"], mesh.shape["dp"]
    far, near, side, core = sizes = 2, columns // 2, replicas // 2, 2

    def step(grads, check_weights):
        rows, width = grads.shape[2:]
        blocks = check_weights.shape[2]
        tiled = (
            width == columns * replicas * LANES
            and rows == LANES
            and blocks == SUBLANES
            and columns == far * near
            and replicas == side * core
            and near & (near - 1) == 0
            and replicas & (replicas - 1) == 0
        )
        if tiled:
            axes = ("far", "near", "side", "core")
            body, used = functools.partial(small_body, sizes), Mesh(mesh.devices.reshape(sizes), axes)
            dp, rep = axes[:2], axes[2:]
        else:
            body, used, dp, rep = large_body, mesh, "dp", "rep"
        placed = P(rep, dp, None, None)
        return jax.shard_map(
            body,
            mesh=used,
            in_specs=(placed, placed),
            out_specs=(P(None, dp), P(None, dp)),
            check_vma=False,
        )(grads, check_weights)

    return step
```

```python
import functools

import jax
import jax.numpy as jnp
from jax import lax
from jax.experimental import pallas as pl
from jax.experimental.pallas import tpu as pltpu
from jax.sharding import Mesh
from jax.sharding import PartitionSpec as P

LANES = 128
SUBLANES = 8
FULL = 32767.0
LEAST, MOST = -126, 126
GRANT = pltpu.CompilerParams(vmem_limit_bytes=8 * 1024 * 1024)


def clip_factor(square, total_rows, width):
    return jnp.minimum(
        1.0, 2.0 * jnp.sqrt(jnp.float32(total_rows * width)) / jnp.sqrt(square + 1e-06)
    )


def pack_kernel(mine, grads_hbm, weights_hbm, out_ref, weights_ref, grads_sem, weights_sem):
    core = lax.axis_index("core")
    target = core if mine else 1 - core
    rows, width = grads_hbm.shape
    blocks, block = weights_ref.shape
    cols = out_ref.shape[1]
    chips = width // (4 * cols)
    fetch = pltpu.make_async_copy(weights_hbm, weights_ref, weights_sem)
    fetch.start()
    copies = []
    for chip in range(chips):
        for half in range(2):
            at = pl.multiple_of(((half * chips + chip) * 2 + target) * cols, cols)
            copies.append(
                pltpu.make_async_copy(
                    grads_hbm.at[:, pl.ds(at, cols)],
                    out_ref.at[pl.ds((chip * 2 + half) * rows, rows), :],
                    grads_sem,
                )
            )
            copies[-1].start()
    fetch.wait()
    place = lax.broadcasted_iota(jnp.int32, (block, rows), 1)
    spread = (place % block == lax.broadcasted_iota(jnp.int32, (block, rows), 0)).astype(jnp.bfloat16)
    repeated = jnp.dot(
        weights_ref[...].astype(jnp.bfloat16), spread, preferred_element_type=jnp.float32
    )
    owner = lax.broadcasted_iota(jnp.int32, (blocks, rows), 1) // block
    own = owner == lax.broadcasted_iota(jnp.int32, (blocks, rows), 0)
    out_ref[pl.ds(2 * chips * rows, blocks), :] = jnp.where(own, repeated, 0.0).astype(jnp.bfloat16)
    for copy in copies:
        copy.wait()


def encode(values):
    top = jnp.maximum(jnp.max(jnp.abs(values), axis=0, keepdims=True), 2.0**LEAST)
    power = jnp.clip(jnp.ceil(jnp.log2(top)), float(LEAST), float(MOST))
    codes = jnp.round(values * jnp.exp2(-power) * FULL)
    return jnp.clip(codes, -FULL, FULL).astype(jnp.int32), power.astype(jnp.int32)


def decode(codes, power):
    values = codes.astype(jnp.int32).astype(jnp.float32) * (1.0 / FULL)
    return values * jnp.exp2(power.astype(jnp.float32))


def shares_of(weights):
    weights = weights.astype(jnp.float32)
    share = weights / jnp.sum(weights, axis=1, keepdims=True)
    high = share.astype(jnp.bfloat16).astype(jnp.float32)
    rest = share - high
    middle = rest.astype(jnp.bfloat16).astype(jnp.float32)
    low = rest - middle
    terms = jnp.concatenate([high, middle, low, jnp.zeros_like(low)], axis=0)
    return terms.astype(jnp.bfloat16)


def place_of(chip, chips):
    return chip ^ (chips - 2)


def checks_of(shares, data):
    blocks = shares.shape[0] // 4
    check = jnp.dot(shares, data, preferred_element_type=jnp.float32)
    return check[:blocks] + check[blocks : 2 * blocks] + check[2 * blocks : 3 * blocks]


def check_kernel(rows, mine_ref, check_ref):
    count = mine_ref.shape[0] // rows
    blocks = mine_ref.shape[0] - count * rows
    shares = shares_of(mine_ref[pl.ds(count * rows, blocks), :])
    for i in range(count):
        check_ref[pl.ds(i * blocks, blocks), :] = checks_of(shares, mine_ref[pl.ds(i * rows, rows), :])


def pair_kernel(rows, mine_ref, check_ref, came_ref, out_ref):
    chips, held, cols = out_ref.shape
    blocks = mine_ref.shape[0] - 2 * chips * rows
    shares = shares_of(came_ref[pl.ds(2 * chips * rows, blocks), :])
    for chip in range(chips):
        powers = []
        place = place_of(chip, chips)
        for half in range(2):
            i = chip * 2 + half
            at = pl.ds(i * rows, rows)
            first, second = mine_ref[at, :], came_ref[at, :]
            check = check_ref[pl.ds(i * blocks, blocks), :] + checks_of(shares, second)
            codes, power = encode(first.astype(jnp.float32) + second.astype(jnp.float32))
            out_ref[place, pl.ds(half * (rows + blocks), rows), :] = codes.astype(jnp.int16)
            powers.append(power)
            codes, power = encode(check)
            out_ref[place, pl.ds(half * (rows + blocks) + rows, blocks), :] = codes.astype(jnp.int16)
            powers.append(power)
        powers.append(jnp.zeros((SUBLANES - 4, cols), jnp.int32))
        out_ref[place, pl.ds(held - SUBLANES, SUBLANES), :] = jnp.concatenate(powers, axis=0).astype(
            jnp.int16
        )


def add_up(rows, blocks, half, recv_ref):
    chips, held, cols = recv_ref.shape
    total = jnp.zeros((rows, cols), jnp.float32)
    check = jnp.zeros((blocks, cols), jnp.float32)
    start = pl.multiple_of(half * (rows + blocks), SUBLANES)
    for chip in range(chips):
        powers = recv_ref[chip, pl.ds(held - SUBLANES, SUBLANES), :].astype(jnp.int32)
        powers = jnp.where(half == 0, powers[:2], powers[2:4])
        total += decode(recv_ref[chip, pl.ds(start, rows), :], powers[:1])
        check += decode(recv_ref[chip, pl.ds(start + rows, blocks), :], powers[1:])
    return total, check


def sum_kernel(rows, blocks, recv_ref, out_ref, mine_ref, other_ref):
    far = lax.axis_index("far")
    other, other_check = add_up(rows, blocks, 1 - far, recv_ref)
    mine, mine_check = add_up(rows, blocks, far, recv_ref)
    powers, start = [], 0
    for values in (other, other_check, mine):
        codes, power = encode(values)
        out_ref[pl.ds(start, values.shape[0]), :] = codes.astype(jnp.int16)
        powers.append(power)
        start += values.shape[0]
    powers.append(jnp.zeros((SUBLANES - len(powers), out_ref.shape[1]), jnp.int32))
    out_ref[pl.ds(start, SUBLANES), :] = jnp.concatenate(powers, axis=0).astype(jnp.int16)
    mine_ref[pl.ds(0, rows), :] = mine
    mine_ref[pl.ds(rows, blocks), :] = mine_check
    other_ref[...] = other


def join_kernel(rows, blocks, mine_ref, other_ref, came_ref, total_ref, square_ref):
    held = rows + blocks
    powers = came_ref[pl.ds(held + rows, SUBLANES), :].astype(jnp.int32)
    total = mine_ref[pl.ds(0, rows), :] + decode(came_ref[pl.ds(0, rows), :], powers[:1])
    other = other_ref[...] + decode(came_ref[pl.ds(held, rows), :], powers[2:3])
    square_ref[...] = jnp.broadcast_to(
        jnp.sum(total * total + other * other, axis=0, keepdims=True), square_ref.shape
    )
    total_ref[pl.ds(0, rows), :] = total
    total_ref[pl.ds(rows, blocks), :] = mine_ref[pl.ds(rows, blocks), :] + decode(
        came_ref[pl.ds(rows, blocks), :], powers[1:2]
    )


def scale_kernel(rows, width, squares_ref, *refs):
    *total_refs, reduced_ref, check_ref = refs
    cols = total_refs[0].shape[1]
    factor = clip_factor(jnp.sum(squares_ref[...], keepdims=True), rows, width)
    me = lax.axis_index("side") * 2 + lax.axis_index("core")
    for step, total_ref in enumerate(total_refs):
        at = pl.ds(pl.multiple_of((me ^ step) * cols, cols), cols)
        scaled = (total_ref[...] * factor).astype(jnp.bfloat16)
        reduced_ref[:, at] = scaled[:rows]
        check_ref[:, at] = scaled[rows:]


def small_body(sizes, grads, check_weights):
    far, near, side, core = sizes
    local, weights = grads[0, 0], check_weights[0, 0]
    rows, width = local.shape
    blocks = weights.shape[0]
    chips, replicas = near * side, side * core
    cols = width // (far * chips * core)
    vmem = pl.BlockSpec(memory_space=pltpu.VMEM)
    hbm = pl.BlockSpec(memory_space=pltpu.HBM)
    sums = jax.ShapeDtypeStruct((rows + blocks, cols), jnp.float32)
    local = pltpu.with_memory_space_constraint(local, pltpu.HBM)
    weights = pltpu.with_memory_space_constraint(weights, pltpu.HBM)

    def pack(mine):
        return pl.pallas_call(
            functools.partial(pack_kernel, mine),
            out_shape=jax.ShapeDtypeStruct((far * chips * rows + blocks, cols), jnp.bfloat16),
            in_specs=[hbm, hbm],
            out_specs=vmem,
            scratch_shapes=[
                pltpu.VMEM(weights.shape, weights.dtype),
                pltpu.SemaphoreType.DMA,
                pltpu.SemaphoreType.DMA,
            ],
            compiler_params=GRANT,
        )(local, weights)

    def call(kernel, out_shape, *operands):
        return pl.pallas_call(
            kernel,
            out_shape=out_shape,
            in_specs=[vmem] * len(operands),
            out_specs=jax.tree.map(lambda _: vmem, out_shape),
            compiler_params=GRANT,
        )(*operands)

    packed = pack(False)
    came = lax.ppermute(packed, "core", [(0, 1), (1, 0)])
    mine = pack(True)
    checks = call(
        functools.partial(check_kernel, rows), jax.ShapeDtypeStruct((far * chips * blocks, cols), jnp.float32), mine
    )
    coded = call(
        functools.partial(pair_kernel, rows),
        jax.ShapeDtypeStruct((chips, far * (rows + blocks) + SUBLANES, cols), jnp.int16),
        mine,
        checks,
        came,
    )
    order = [[place_of(chip, chips) for chip in range(chips)]]
    received = lax.all_to_all(
        coded, ("near", "side"), 0, 0, tiled=True, axis_index_groups=order
    )
    part = jax.ShapeDtypeStruct((rows, cols), jnp.float32)
    codes, mine, other = call(
        functools.partial(sum_kernel, rows, blocks),
        (jax.ShapeDtypeStruct((2 * rows + blocks + SUBLANES, cols), jnp.int16), sums, part),
        received,
    )
    came = lax.ppermute(codes, "far", [(0, 1), (1, 0)])
    total, square = call(
        functools.partial(join_kernel, rows, blocks),
        (sums, jax.ShapeDtypeStruct((chips * core, cols), jnp.float32)),
        mine,
        other,
        came,
    )
    totals = [total]
    for step in range(1, replicas):
        swaps = [(i, i ^ step) for i in range(replicas)]
        totals.append(lax.ppermute(total, ("side", "core"), swaps))
    backward = [list(range(chips * core))[::-1]]
    squares = lax.all_to_all(
        square, ("near", "side", "core"), 0, 0, tiled=True, axis_index_groups=backward
    )
    wide = replicas * cols
    return call(
        functools.partial(scale_kernel, rows, width),
        (
            jax.ShapeDtypeStruct((rows, wide), jnp.bfloat16),
            jax.ShapeDtypeStruct((blocks, wide), jnp.bfloat16),
        ),
        squares,
        *totals,
    )


def large_body(grads, check_weights):
    local, weights = grads[0, 0], check_weights[0, 0]
    rows, width = local.shape
    blocks, block = weights.shape
    wsum = jnp.sum(weights, axis=-1).astype(jnp.float32)
    local_check = jnp.einsum(
        "kb,kbe->ke",
        weights.astype(jnp.bfloat16),
        local.reshape(blocks, block, width),
        preferred_element_type=jnp.float32,
    )
    terms = jnp.concatenate([local.astype(jnp.float32), local_check / wsum[:, None]], axis=0)
    owned = lax.psum(lax.psum_scatter(terms, "dp", scatter_dimension=1, tiled=True), "rep")
    square = lax.psum(jnp.sum(owned[:rows] * owned[:rows]), "dp")
    scaled = (clip_factor(square, rows, width) * owned).astype(jnp.bfloat16)
    return scaled[:rows], scaled[rows:]


def solution(mesh):
    replicas, columns = mesh.shape["rep"], mesh.shape["dp"]
    far, near, side, core = sizes = 2, columns // 2, replicas // 2, 2

    def step(grads, check_weights):
        rows, width = grads.shape[2:]
        blocks = check_weights.shape[2]
        tiled = (
            width == columns * replicas * LANES
            and rows == LANES
            and blocks == SUBLANES
            and columns == far * near
            and replicas == side * core
            and near & (near - 1) == 0
            and replicas & (replicas - 1) == 0
        )
        if tiled:
            axes = ("far", "near", "side", "core")
            body, used = functools.partial(small_body, sizes), Mesh(mesh.devices.reshape(sizes), axes)
            dp, rep = axes[:2], axes[2:]
        else:
            body, used, dp, rep = large_body, mesh, "dp", "rep"
        placed = P(rep, dp, None, None)
        return jax.shard_map(
            body,
            mesh=used,
            in_specs=(placed, placed),
            out_specs=(P(None, dp), P(None, dp)),
            check_vma=False,
        )(grads, check_weights)

    return step
```

```python
import functools

import jax
import jax.numpy as jnp
from jax import lax
from jax.experimental import pallas as pl
from jax.experimental.pallas import tpu as pltpu
from jax.sharding import Mesh
from jax.sharding import PartitionSpec as P

LANES = 128
SUBLANES = 8
FULL = 32767.0
LEAST, MOST = -126, 126
STEPS = 128
GRANT = pltpu.CompilerParams(vmem_limit_bytes=8 * 1024 * 1024)


def clip_factor(square, total_rows, width):
    return jnp.minimum(
        1.0, 2.0 * jnp.sqrt(jnp.float32(total_rows * width)) / jnp.sqrt(square + 1e-06)
    )


def pack_kernel(mine, grads_hbm, weights_hbm, out_ref, weights_ref, grads_sem, weights_sem):
    core = lax.axis_index("core")
    target = core if mine else 1 - core
    rows, width = grads_hbm.shape
    blocks, block = weights_ref.shape
    cols = out_ref.shape[1]
    chips = width // (4 * cols)
    fetch = pltpu.make_async_copy(weights_hbm, weights_ref, weights_sem)
    fetch.start()
    copies = []
    for chip in range(chips):
        for half in range(2):
            at = pl.multiple_of(((half * chips + chip) * 2 + target) * cols, cols)
            copies.append(
                pltpu.make_async_copy(
                    grads_hbm.at[:, pl.ds(at, cols)],
                    out_ref.at[pl.ds((chip * 2 + half) * rows, rows), :],
                    grads_sem,
                )
            )
            copies[-1].start()
    fetch.wait()
    place = lax.broadcasted_iota(jnp.int32, (block, rows), 1)
    spread = (place % block == lax.broadcasted_iota(jnp.int32, (block, rows), 0)).astype(jnp.bfloat16)
    repeated = jnp.dot(
        weights_ref[...].astype(jnp.bfloat16), spread, preferred_element_type=jnp.float32
    )
    owner = lax.broadcasted_iota(jnp.int32, (blocks, rows), 1) // block
    own = owner == lax.broadcasted_iota(jnp.int32, (blocks, rows), 0)
    out_ref[pl.ds(2 * chips * rows, blocks), :] = jnp.where(own, repeated, 0.0).astype(jnp.bfloat16)
    for copy in copies:
        copy.wait()


def encode(values):
    top = jnp.maximum(jnp.max(jnp.abs(values), axis=0, keepdims=True), 2.0**LEAST)
    power = jnp.clip(jnp.ceil(jnp.log2(top) * STEPS), float(LEAST * STEPS), float(MOST * STEPS))
    codes = jnp.round(values * jnp.exp2(power * (-1.0 / STEPS)) * FULL)
    return jnp.clip(codes, -FULL, FULL).astype(jnp.int32), power.astype(jnp.int32)


def decode(codes, power):
    values = codes.astype(jnp.int32).astype(jnp.float32) * (1.0 / FULL)
    return values * jnp.exp2(power.astype(jnp.float32) * (1.0 / STEPS))


def shares_of(weights):
    weights = weights.astype(jnp.float32)
    share = weights / jnp.sum(weights, axis=1, keepdims=True)
    high = share.astype(jnp.bfloat16).astype(jnp.float32)
    rest = share - high
    middle = rest.astype(jnp.bfloat16).astype(jnp.float32)
    low = rest - middle
    terms = jnp.concatenate([high, middle, low, jnp.zeros_like(low)], axis=0)
    return terms.astype(jnp.bfloat16)


def place_of(chip, chips):
    return chip ^ (chips - 2)


def checks_of(shares, data):
    blocks = shares.shape[0] // 4
    check = jnp.dot(shares, data, preferred_element_type=jnp.float32)
    return check[:blocks] + check[blocks : 2 * blocks] + check[2 * blocks : 3 * blocks]


def check_kernel(rows, mine_ref, check_ref):
    count = mine_ref.shape[0] // rows
    blocks = mine_ref.shape[0] - count * rows
    shares = shares_of(mine_ref[pl.ds(count * rows, blocks), :])
    for i in range(count):
        check_ref[pl.ds(i * blocks, blocks), :] = checks_of(shares, mine_ref[pl.ds(i * rows, rows), :])


def pair_kernel(rows, mine_ref, check_ref, came_ref, out_ref):
    chips, held, cols = out_ref.shape
    blocks = mine_ref.shape[0] - 2 * chips * rows
    shares = shares_of(came_ref[pl.ds(2 * chips * rows, blocks), :])
    for chip in range(chips):
        powers = []
        place = place_of(chip, chips)
        for half in range(2):
            i = chip * 2 + half
            at = pl.ds(i * rows, rows)
            first, second = mine_ref[at, :], came_ref[at, :]
            check = check_ref[pl.ds(i * blocks, blocks), :] + checks_of(shares, second)
            codes, power = encode(first.astype(jnp.float32) + second.astype(jnp.float32))
            out_ref[place, pl.ds(half * (rows + blocks), rows), :] = codes.astype(jnp.int16)
            powers.append(power)
            codes, power = encode(check)
            out_ref[place, pl.ds(half * (rows + blocks) + rows, blocks), :] = codes.astype(jnp.int16)
            powers.append(power)
        powers.append(jnp.zeros((SUBLANES - 4, cols), jnp.int32))
        out_ref[place, pl.ds(held - SUBLANES, SUBLANES), :] = jnp.concatenate(powers, axis=0).astype(
            jnp.int16
        )


def add_up(rows, blocks, half, recv_ref):
    chips, held, cols = recv_ref.shape
    total = jnp.zeros((rows, cols), jnp.float32)
    check = jnp.zeros((blocks, cols), jnp.float32)
    start = pl.multiple_of(half * (rows + blocks), SUBLANES)
    for chip in range(chips):
        powers = recv_ref[chip, pl.ds(held - SUBLANES, SUBLANES), :].astype(jnp.int32)
        powers = jnp.where(half == 0, powers[:2], powers[2:4])
        total += decode(recv_ref[chip, pl.ds(start, rows), :], powers[:1])
        check += decode(recv_ref[chip, pl.ds(start + rows, blocks), :], powers[1:])
    return total, check


def sum_kernel(rows, blocks, recv_ref, out_ref, mine_ref, other_ref):
    far = lax.axis_index("far")
    other, other_check = add_up(rows, blocks, 1 - far, recv_ref)
    mine, mine_check = add_up(rows, blocks, far, recv_ref)
    powers, start = [], 0
    for values in (other, other_check, mine):
        codes, power = encode(values)
        out_ref[pl.ds(start, values.shape[0]), :] = codes.astype(jnp.int16)
        powers.append(power)
        start += values.shape[0]
    powers.append(jnp.zeros((SUBLANES - len(powers), out_ref.shape[1]), jnp.int32))
    out_ref[pl.ds(start, SUBLANES), :] = jnp.concatenate(powers, axis=0).astype(jnp.int16)
    mine_ref[pl.ds(0, rows), :] = mine
    mine_ref[pl.ds(rows, blocks), :] = mine_check
    other_ref[...] = other


def join_kernel(rows, blocks, mine_ref, other_ref, came_ref, total_ref, square_ref):
    held = rows + blocks
    powers = came_ref[pl.ds(held + rows, SUBLANES), :].astype(jnp.int32)
    total = mine_ref[pl.ds(0, rows), :] + decode(came_ref[pl.ds(0, rows), :], powers[:1])
    other = other_ref[...] + decode(came_ref[pl.ds(held, rows), :], powers[2:3])
    square_ref[...] = jnp.broadcast_to(
        jnp.sum(total * total + other * other, axis=0, keepdims=True), square_ref.shape
    )
    total_ref[pl.ds(0, rows), :] = total
    total_ref[pl.ds(rows, blocks), :] = mine_ref[pl.ds(rows, blocks), :] + decode(
        came_ref[pl.ds(rows, blocks), :], powers[1:2]
    )


def scale_kernel(rows, width, squares_ref, *refs):
    *total_refs, reduced_ref, check_ref = refs
    cols = total_refs[0].shape[1]
    factor = clip_factor(jnp.sum(squares_ref[...], keepdims=True), rows, width)
    me = lax.axis_index("side") * 2 + lax.axis_index("core")
    for step, total_ref in enumerate(total_refs):
        at = pl.ds(pl.multiple_of((me ^ step) * cols, cols), cols)
        scaled = (total_ref[...] * factor).astype(jnp.bfloat16)
        reduced_ref[:, at] = scaled[:rows]
        check_ref[:, at] = scaled[rows:]


def small_body(sizes, grads, check_weights):
    far, near, side, core = sizes
    local, weights = grads[0, 0], check_weights[0, 0]
    rows, width = local.shape
    blocks = weights.shape[0]
    chips, replicas = near * side, side * core
    cols = width // (far * chips * core)
    vmem = pl.BlockSpec(memory_space=pltpu.VMEM)
    hbm = pl.BlockSpec(memory_space=pltpu.HBM)
    sums = jax.ShapeDtypeStruct((rows + blocks, cols), jnp.float32)
    local = pltpu.with_memory_space_constraint(local, pltpu.HBM)
    weights = pltpu.with_memory_space_constraint(weights, pltpu.HBM)

    def pack(mine):
        return pl.pallas_call(
            functools.partial(pack_kernel, mine),
            out_shape=jax.ShapeDtypeStruct((far * chips * rows + blocks, cols), jnp.bfloat16),
            in_specs=[hbm, hbm],
            out_specs=vmem,
            scratch_shapes=[
                pltpu.VMEM(weights.shape, weights.dtype),
                pltpu.SemaphoreType.DMA,
                pltpu.SemaphoreType.DMA,
            ],
            compiler_params=GRANT,
        )(local, weights)

    def call(kernel, out_shape, *operands):
        return pl.pallas_call(
            kernel,
            out_shape=out_shape,
            in_specs=[vmem] * len(operands),
            out_specs=jax.tree.map(lambda _: vmem, out_shape),
            compiler_params=GRANT,
        )(*operands)

    packed = pack(False)
    came = lax.ppermute(packed, "core", [(0, 1), (1, 0)])
    mine = pack(True)
    checks = call(
        functools.partial(check_kernel, rows), jax.ShapeDtypeStruct((far * chips * blocks, cols), jnp.float32), mine
    )
    coded = call(
        functools.partial(pair_kernel, rows),
        jax.ShapeDtypeStruct((chips, far * (rows + blocks) + SUBLANES, cols), jnp.int16),
        mine,
        checks,
        came,
    )
    order = [[place_of(chip, chips) for chip in range(chips)]]
    received = lax.all_to_all(
        coded, ("near", "side"), 0, 0, tiled=True, axis_index_groups=order
    )
    part = jax.ShapeDtypeStruct((rows, cols), jnp.float32)
    codes, mine, other = call(
        functools.partial(sum_kernel, rows, blocks),
        (jax.ShapeDtypeStruct((2 * rows + blocks + SUBLANES, cols), jnp.int16), sums, part),
        received,
    )
    came = lax.ppermute(codes, "far", [(0, 1), (1, 0)])
    total, square = call(
        functools.partial(join_kernel, rows, blocks),
        (sums, jax.ShapeDtypeStruct((chips * core, cols), jnp.float32)),
        mine,
        other,
        came,
    )
    totals = [total]
    for step in range(1, replicas):
        swaps = [(i, i ^ step) for i in range(replicas)]
        totals.append(lax.ppermute(total, ("side", "core"), swaps))
    backward = [list(range(chips * core))[::-1]]
    squares = lax.all_to_all(
        square, ("near", "side", "core"), 0, 0, tiled=True, axis_index_groups=backward
    )
    wide = replicas * cols
    return call(
        functools.partial(scale_kernel, rows, width),
        (
            jax.ShapeDtypeStruct((rows, wide), jnp.bfloat16),
            jax.ShapeDtypeStruct((blocks, wide), jnp.bfloat16),
        ),
        squares,
        *totals,
    )


def large_body(grads, check_weights):
    local, weights = grads[0, 0], check_weights[0, 0]
    rows, width = local.shape
    blocks, block = weights.shape
    wsum = jnp.sum(weights, axis=-1).astype(jnp.float32)
    local_check = jnp.einsum(
        "kb,kbe->ke",
        weights.astype(jnp.bfloat16),
        local.reshape(blocks, block, width),
        preferred_element_type=jnp.float32,
    )
    terms = jnp.concatenate([local.astype(jnp.float32), local_check / wsum[:, None]], axis=0)
    owned = lax.psum(lax.psum_scatter(terms, "dp", scatter_dimension=1, tiled=True), "rep")
    square = lax.psum(jnp.sum(owned[:rows] * owned[:rows]), "dp")
    scaled = (clip_factor(square, rows, width) * owned).astype(jnp.bfloat16)
    return scaled[:rows], scaled[rows:]


def solution(mesh):
    replicas, columns = mesh.shape["rep"], mesh.shape["dp"]
    far, near, side, core = sizes = 2, columns // 2, replicas // 2, 2

    def step(grads, check_weights):
        rows, width = grads.shape[2:]
        blocks = check_weights.shape[2]
        tiled = (
            width == columns * replicas * LANES
            and rows == LANES
            and blocks == SUBLANES
            and columns == far * near
            and replicas == side * core
            and near & (near - 1) == 0
            and replicas & (replicas - 1) == 0
        )
        if tiled:
            axes = ("far", "near", "side", "core")
            body, used = functools.partial(small_body, sizes), Mesh(mesh.devices.reshape(sizes), axes)
            dp, rep = axes[:2], axes[2:]
        else:
            body, used, dp, rep = large_body, mesh, "dp", "rep"
        placed = P(rep, dp, None, None)
        return jax.shard_map(
            body,
            mesh=used,
            in_specs=(placed, placed),
            out_specs=(P(None, dp), P(None, dp)),
            check_vma=False,
        )(grads, check_weights)

    return step
```
